32 devices in a mesh: batch: 4 (over y, x), seq: 4 (over z), head: 2 (over core).
Axes of the slice: x: 2, y: 2, z: 4, core: 2. Of those that a mesh axis runs over, the one named last changes fastest.
Arguments:
- queries: bfloat16 [1, 6144, 2048], P(None, ('batch', 'seq'), 'head'), parts along dimension 1, may hold values from -240 to 240
- keys: bfloat16 [1, 6144, 1024], P(None, ('batch', 'seq'), 'head'), parts along dimension 1, may hold values from -6 to 6
- values: bfloat16 [1, 6144, 1024], P(None, ('batch', 'seq'), 'head'), parts along dimension 1, may hold values from -6 to 6
- exit_layer: int32 [48], P(('batch', 'seq')), parts along dimension 0, may hold values from 0 to 1
- tile_order: int32 [48], P('batch'), parts along dimension 0, may hold values from 0 to 11, each once
Outputs:
- attended: bfloat16 [1, 6144, 2048], P(None, ('batch', 'seq'), 'head'), parts along dimension 1
- live_tiles: int32 [4], P('batch'), parts along dimension 0
The draws below stay inside these ranges and needn't reach their ends.
There are 4 independent parts, one for each index of `batch`. The reference program is written for one: setup_inputs(seed, part) draws one part's arguments, and reference() takes and returns one part's arrays. A program takes and returns all parts, laid end to end along the dimension named above; each array names one. Nothing has to cross between parts.
Inputs may be any that keep to these rules, and one draw needn't show every extreme that they name: Tile t covers tokens t * 128 to t * 128 + 127 of the token dimension; tile_order is a permutation of 0 to 11.
All inputs are finite; a program needn't handle non-finite values.
Results may differ from the reference program's by a relative error of at most 0.0049.
Values may be sent and summed in bfloat16 or wider, within the bound.
A program may use at most 128 MiB of HBM per device.

```python
import math
import jax
import jax.numpy as jnp
from jax import lax

LAYERS = 1
QH = 8
KVH = 4
HD = 256
TILE = 128
TOKENS = 1536
TILES = 12
KW = 1024


def draw_queries(key, part):
    query_key = jax.random.fold_in(key, 101)
    base = jnp.clip(jax.random.normal(query_key, (LAYERS, TOKENS, QH * HD), jnp.float32), -6.0, 6.0)
    return base.astype(jnp.bfloat16)


def draw_exit_layer(key, part):
    exit_key = jax.random.fold_in(key, 202)
    tile_ids = jnp.arange(TILES, dtype=jnp.int32)
    lowest = tile_ids * LAYERS // TILES
    spread = LAYERS + 1 - lowest
    raw_bits = jax.random.randint(exit_key, (TILES,), 0, 1 << 20, dtype=jnp.int32)
    return (lowest + raw_bits % spread).astype(jnp.int32)


def levels(own_key, shape, pieces, low, largest):
    def one(dim, parts):
        draws = jax.random.uniform(jax.random.fold_in(jax.random.fold_in(own_key, 6), dim), (parts,), jnp.float32, low / len(pieces), largest / len(pieces))
        return jnp.repeat(jnp.exp(draws), shape[dim] // parts).reshape((-1,) + (1,) * (len(shape) - dim - 1))

    gain = one(*pieces[0])
    for cut in pieces[1:]:
        gain = gain * one(*cut)
    return gain


def bell_draw(own_key, shape, width, reach, shards=(), held_as=jnp.bfloat16):
    drawn = width * jax.random.normal(own_key, shape, jnp.float32)
    if shards:
        drawn = drawn * levels(own_key, shape, shards, -0.22, 0.18)
    return jnp.clip(drawn, -reach, reach).astype(held_as)


def setup_inputs(seed: int = 0, part: int = 0) -> dict:
    streams_of = jax.random.split(jax.random.key(seed), 6)
    part_keys = jax.random.split(jax.random.fold_in(streams_of[5], part), 6)
    queries = draw_queries(jax.random.fold_in(jax.random.fold_in(streams_of[5], part), 71), part)
    keys = bell_draw(part_keys[1], (LAYERS, TOKENS, KW), 1.0, 6.0, ((1, 4), (2, 2)))
    values = bell_draw(part_keys[2], (LAYERS, TOKENS, KW), 1.0, 6.0, ((1, 4), (2, 2)))
    exit_layer = draw_exit_layer(jax.random.fold_in(jax.random.fold_in(streams_of[5], part), 71), part)
    tile_order = jax.random.permutation(part_keys[4], TILES).astype(jnp.int32)
    return dict(queries=queries, keys=keys, values=values, exit_layer=exit_layer, tile_order=tile_order)


softcap = 50.0
query_scale = 0.0625


def reference(queries, keys, values, exit_layer, tile_order):
    group_size = QH // KVH
    offsets = jnp.arange(TOKENS, dtype=jnp.int32)
    positions = (tile_order[offsets // TILE] * TILE + offsets % TILE).astype(jnp.int32)
    token_exits = exit_layer[offsets // TILE]
    block_rows = math.gcd(TOKENS, 512)
    outputs = []
    for layer_id in range(LAYERS):
        key_heads = keys[layer_id].reshape(TOKENS, KVH, HD).astype(jnp.float32)
        value_heads = values[layer_id].reshape(TOKENS, KVH, HD).astype(jnp.float32)
        query_blocks = queries[layer_id].reshape(TOKENS // block_rows, block_rows, KVH, group_size, HD)
        query_pos = positions.reshape(TOKENS // block_rows, block_rows)

        def one_block(operands):
            query_block, pos_block = operands
            scores = jnp.einsum("tkgd,skd->kgts", query_block.astype(jnp.float32), key_heads) * query_scale
            allowed = positions[None, :] <= pos_block[:, None]
            weights = jnp.where(allowed[None, None], jnp.exp(softcap * jnp.tanh(scores / softcap)), 0.0)
            denominator = jnp.sum(weights, axis=-1)
            rounded = lax.optimization_barrier(weights.astype(jnp.bfloat16))
            numerator = jnp.einsum("kgts,skd->kgtd", rounded.astype(jnp.float32), value_heads)
            output = numerator / denominator[..., None]
            return jnp.transpose(output, (2, 0, 1, 3)).reshape(block_rows, QH * HD)

        attended_layer = lax.map(one_block, (query_blocks, query_pos)).reshape(TOKENS, QH * HD)
        attended_layer = jnp.where((token_exits > layer_id)[:, None], attended_layer, 0.0)
        outputs.append(attended_layer.astype(jnp.bfloat16))
    live_tiles = jnp.stack([jnp.sum((exit_layer > layer_id).astype(jnp.int32)) for layer_id in range(LAYERS)])
    return jnp.stack(outputs), live_tiles.astype(jnp.int32)
```

```python
import functools
import math

import jax
import jax.numpy as jnp
from jax import lax
from jax.experimental import pallas as pl
from jax.experimental.pallas import tpu as pltpu
from jax.sharding import PartitionSpec as P

HD = 256
TILE = 128
SOFTCAP = 50.0
QUERY_SCALE = 0.0625
IN_SCALE = QUERY_SCALE / SOFTCAP
OUT_SCALE = SOFTCAP * math.log2(math.e)
MESH = pl.DeviceIdType.MESH
SERVED, SPREAD = 0, 1


def kernel(
    n, order_ref, exit_ref, q_hbm, k_hbm, v_hbm, out_ref, live_ref,
    qb, kv, acc, den, done, exits, kv_sem, q_sem, send_sem, recv_sem,
    pair_send, pair_recv, exit_send, exit_recv,
):
    me = lax.axis_index("seq")
    core = lax.axis_index("head")
    tiles = kv.shape[2]
    heads, rows = qb.shape[1:3]
    q_half = heads * HD
    far = n - 1
    at_end = (me == 0) | (me == far)
    serves = (me == 1) | (me == far - 1)
    end = jnp.where(me < n // 2, 0, far)
    inward = jnp.where(me < n // 2, 1, -1)
    first = core

    def inside(owner):
        return (owner >= 0) & (owner < n)

    def peer(step):
        return {"seq": jnp.clip(me + step, 0, far)}

    def own_copy(hh, which):
        src = (k_hbm, v_hbm)[which]
        return pltpu.make_async_copy(
            src.at[:, :, pl.ds(pl.multiple_of(hh * HD, HD), HD)],
            kv.at[me, hh, :, which],
            kv_sem.at[hh, which],
        )

    def own_queries(hh, h):
        return pltpu.make_async_copy(
            q_hbm.at[:, pl.ds(hh * q_half + h * HD, HD)], qb.at[hh, h], q_sem.at[hh, h]
        )

    barrier = pltpu.get_barrier_semaphore()
    for step in (1, -1):
        @pl.when(inside(me + step))
        def _():
            pl.semaphore_signal(barrier, inc=1, device_id=peer(step), device_id_type=MESH)

    for which in range(2):
        own_copy(first, which).start()
    for h in range(heads):
        own_queries(0, h).start()
    for which in range(2):
        own_copy(1 - first, which).start()
    for h in range(heads):
        own_queries(1, h).start()

    lane = lax.broadcasted_iota(jnp.int32, (1, TILE), 1)
    mine = jnp.zeros((1, TILE), jnp.int32)
    for i in range(tiles):
        mine = jnp.where(lane == i, exit_ref[i], mine)
    exits[me] = mine

    pl.semaphore_wait(barrier, jnp.where(at_end, 1, 2))

    def hop(owner, hh, t, step):
        return pltpu.make_async_remote_copy(
            src_ref=kv.at[owner, hh, t],
            dst_ref=kv.at[owner, hh, t],
            send_sem=send_sem.at[jnp.where((owner == me) & (step < 0), n, owner), hh, t],
            recv_sem=recv_sem.at[owner, hh, t],
            device_id=peer(step),
            device_id_type=MESH,
        )

    def exit_hop(owner, step):
        return pltpu.make_async_remote_copy(
            src_ref=exits.at[owner],
            dst_ref=exits.at[owner],
            send_sem=exit_send.at[jnp.where((owner == me) & (step < 0), n, owner)],
            recv_sem=exit_recv.at[owner],
            device_id=peer(step),
            device_id_type=MESH,
        )

    def goes(hh, step):
        room = jnp.where(step > 0, far - me, me)
        return (room > 1) | ((room == 1) & (hh == SPREAD))

    def send(owner, hh, t, step):
        @pl.when(goes(hh, step))
        def _():
            hop(owner, hh, t, step).start()

    def send_own(hh, step):
        @pl.loop(0, tiles)
        def _(t):
            send(me, hh, t, step)

    def query_copy():
        return pltpu.make_async_remote_copy(
            src_ref=qb.at[0], dst_ref=qb.at[2],
            send_sem=pair_send.at[tiles], recv_sem=pair_recv.at[tiles],
            device_id=peer(inward), device_id_type=MESH,
        )

    def done_copy(t):
        part = pl.ds(t * TILE, TILE)
        return pltpu.make_async_remote_copy(
            src_ref=done.at[0, part], dst_ref=done.at[1, part],
            send_sem=pair_send.at[t], recv_sem=pair_recv.at[t],
            device_id=peer(-inward), device_id_type=MESH,
        )

    def wait_own(hh):
        for which in range(2):
            own_copy(hh, which).wait()

    @pl.when(at_end & (core == 0))
    def _():
        for h in range(heads):
            own_queries(0, h).wait()
        query_copy().start()

    wait_own(first)

    @pl.when(~at_end)
    def _():
        send_own(first, inward)
        send_own(first, -inward)

    @pl.when(at_end & (core == 0))
    def _():
        send_own(SERVED, inward)

    wait_own(1 - first)

    @pl.when(~at_end)
    def _():
        send_own(1 - first, -inward)

        @pl.when(core == 1)
        def _():
            send_own(SERVED, inward)

    @pl.when(at_end & (core == 0))
    def _():
        send_own(SPREAD, inward)

    for step in (1, -1):
        @pl.when(inside(me + step))
        def _():
            exit_hop(me, step).start()

    acc[...] = jnp.zeros_like(acc)
    den[...] = jnp.zeros_like(den)

    @pl.when(~(at_end & (core == 0)))
    def _():
        for h in range(heads):
            own_queries(0, h).wait()
    for h in range(heads):
        own_queries(1, h).wait()
    ahead = lax.broadcasted_iota(jnp.int32, (TILE, TILE), 1) - lax.broadcasted_iota(
        jnp.int32, (TILE, TILE), 0
    )

    def fold_into(slot, row_owner, owner, hh, t):
        key_place = order_ref[owner * tiles + t]
        over = jnp.stack(
            [
                ahead - (order_ref[row_owner * tiles + i] - key_place) * TILE
                for i in range(tiles)
            ]
        )
        stacked = (heads * rows, HD)
        scores = lax.dot_general(
            qb[slot].reshape(stacked), kv[owner, hh, t, 0],
            (((1,), (1,)), ((), ())), preferred_element_type=jnp.float32,
        ).reshape(heads, tiles, TILE, TILE)
        weights = jnp.where(
            over[None] <= 0, jnp.exp2(OUT_SCALE * jnp.tanh(scores * IN_SCALE)), 0.0
        ).reshape(heads * rows, TILE)
        den[slot] += weights
        acc[slot] += jnp.dot(
            weights.astype(jnp.bfloat16), kv[owner, hh, t, 1],
            preferred_element_type=jnp.float32,
        )

    def finish(slot, i, h):
        here = pl.ds(h * rows + i * TILE, TILE)
        total = jnp.sum(den[slot, here, :], axis=1, keepdims=True)
        return (acc[slot, here, :] / total).astype(jnp.bfloat16)

    def live_only(i, rows_out):
        return jnp.where(exit_ref[i] > 0, rows_out, jnp.zeros_like(rows_out))

    def keep(slot, i, h):
        out_ref[pl.ds(i * TILE, TILE), pl.ds(slot * q_half + h * HD, HD)] = live_only(
            i, finish(slot, i, h)
        )

    @pl.loop(jnp.where(at_end, tiles * (1 - core), 0), jnp.where(at_end, tiles * (2 - core), 2 * tiles))
    def _(k):
        hh = jnp.where(k < tiles, first, 1 - first)
        fold_into(hh, me, me, hh, lax.rem(k, tiles))

    def arrive(owner, hh, t, side):
        hop(owner, hh, t, side).wait_recv()
        send(owner, hh, t, -side)

        @pl.when((hh == SPREAD) & (t == 0))
        def _():
            exit_hop(owner, side).wait_recv()

            @pl.when(inside(me - side))
            def _():
                exit_hop(owner, -side).start()

    early = core == 0

    @pl.loop(0, 2 * far)
    def _(u):
        hh_in = jnp.where(early, u >= far, (u == 0) | (u > far)).astype(jnp.int32)
        s_in = jnp.where(
            u >= far + 1 - early, u - far + 1, jnp.where(early, u + 1, jnp.maximum(u, 1))
        )
        hh_out = (u >= far).astype(jnp.int32)
        s_out = jnp.where(u >= far, u - far + 1, u + early)
        from_in = me + inward * s_in
        from_out = me - inward * s_out
        has_in = inside(from_in) & ~(at_end & (hh_in == SERVED))
        has_out = inside(from_out) & (s_out > 0) & ~at_end
        serving = serves & (hh_in == SERVED)

        @pl.when(serving & (s_in == 2))
        def _():
            query_copy().wait_recv()

        @pl.loop(0, tiles)
        def _(t):
            @pl.when(at_end & (u == 2 * far - 1) & (t == tiles - 1))
            def _():
                for i in range(tiles):
                    here = pl.ds(i * TILE, TILE)
                    done_copy(i).wait_recv()
                    out_ref[here, pl.ds(0, q_half)] = live_only(i, done[1, here, :])

            @pl.when(has_in)
            def _():
                arrive(from_in, hh_in, t, inward)

            @pl.when(has_out)
            def _():
                arrive(from_out, hh_out, t, -inward)

            @pl.loop(0, 6)
            def _(k):
                near = jnp.where(k == 3, me, jnp.where(k == 4, me + inward, me - inward))
                owner = jnp.where(k > 2, near, jnp.where(k == 1, from_out, from_in))
                runs = jnp.where(
                    k > 2,
                    serving & (s_in == 2),
                    jnp.where(k == 2, serving & has_in & (s_in > 1), jnp.where(k == 1, has_out, has_in)),
                )
                hh = jnp.where(k == 1, hh_out, hh_in)

                @pl.when(runs)
                def _():
                    fold_into(
                        jnp.where(k > 1, 2, hh), jnp.where(k > 1, end, me), owner, hh, t
                    )

        @pl.when((u == 0) & early & ~at_end)
        def _():
            send_own(SPREAD, inward)

        @pl.when((u == 0) & ~early & at_end)
        def _():
            query_copy().start()
            send_own(SERVED, inward)
            send_own(SPREAD, inward)

        @pl.when(serving & (s_in == far - 1))
        def _():
            for t in range(tiles):
                for h in range(heads):
                    done[0, pl.ds(t * TILE, TILE), pl.ds(h * HD, HD)] = finish(2, t, h)
                if t > 0:
                    done_copy(t - 1).start()
            for h in range(heads):
                keep(0, 0, h)
            done_copy(tiles - 1).start()

    for i in range(tiles):
        for h in range(heads):
            keep(1, i, h)

    @pl.when(~at_end)
    def _():
        for i in range(tiles):
            for h in range(heads):
                keep(0, i, h)

    live_ref[0] = jnp.sum((exits[...] > 0).astype(jnp.int32))

    @pl.when(at_end)
    def _():
        query_copy().wait_send()

    @pl.when(serves)
    def _():
        for t in range(tiles):
            done_copy(t).wait_send()

    for step in (1, -1):
        @pl.loop(0, n)
        def _(s):
            owner = me - step * s

            @pl.when(inside(owner) & inside(me + step))
            def _():
                exit_hop(owner, step).wait_send()

            @pl.loop(0, 2)
            def _(hh):
                @pl.when(inside(owner) & goes(hh, step))
                def _():
                    @pl.loop(0, tiles)
                    def _(t):
                        hop(owner, hh, t, step).wait_send()


def body(n, queries, keys, values, exit_layer, tile_order):
    rows, q_width = queries.shape[1:]
    kv_width = keys.shape[2]
    q_half = q_width // 2
    heads = q_half // HD
    tiles = rows // TILE
    smem = pl.BlockSpec(memory_space=pltpu.SMEM)
    hbm = pl.BlockSpec(memory_space=pl.ANY)
    vmem = pl.BlockSpec(memory_space=pltpu.VMEM)
    dma = pltpu.SemaphoreType.DMA
    attended, live = pl.pallas_call(
        functools.partial(kernel, n),
        out_shape=(
            jax.ShapeDtypeStruct((rows, q_width), jnp.bfloat16),
            jax.ShapeDtypeStruct((1,), jnp.int32),
        ),
        in_specs=[smem, smem, hbm, hbm, hbm],
        out_specs=(vmem, smem),
        scratch_shapes=[
            pltpu.VMEM((3, heads, rows, HD), jnp.bfloat16),
            pltpu.VMEM((n, 2, tiles, 2, TILE, HD), jnp.bfloat16),
            pltpu.VMEM((3, heads * rows, HD), jnp.float32),
            pltpu.VMEM((3, heads * rows, TILE), jnp.float32),
            pltpu.VMEM((2, rows, q_half), jnp.bfloat16),
            pltpu.VMEM((n, 1, TILE), jnp.int32),
            dma((2, 2)),
            dma((2, heads)),
            dma((n + 1, 2, tiles)),
            dma((n, 2, tiles)),
            dma((tiles + 1,)),
            dma((tiles + 1,)),
            dma((n + 1,)),
            dma((n,)),
        ],
        compiler_params=pltpu.CompilerParams(
            collective_id=0, has_side_effects=True, vmem_limit_bytes=64_000_000
        ),
        name="attend_line",
    )(
        tile_order, exit_layer, queries[0],
        keys.reshape(tiles, TILE, kv_width), values.reshape(tiles, TILE, kv_width),
    )
    return attended[None], live


def solution(mesh):
    return jax.shard_map(
        functools.partial(body, mesh.shape["seq"]),
        mesh=mesh,
        in_specs=(
            P(None, ("batch", "seq"), "head"),
            P(None, ("batch", "seq"), "head"),
            P(None, ("batch", "seq"), "head"),
            P(("batch", "seq")),
            P("batch"),
        ),
        out_specs=(P(None, ("batch", "seq"), "head"), P("batch")),
        check_vma=False,
    )
```

```python
import functools
import math

import jax
import jax.numpy as jnp
from jax import lax
from jax.experimental import pallas as pl
from jax.experimental.pallas import tpu as pltpu
from jax.sharding import PartitionSpec as P

HD = 256
TILE = 128
SOFTCAP = 50.0
QUERY_SCALE = 0.0625
IN_SCALE = QUERY_SCALE / SOFTCAP
OUT_SCALE = SOFTCAP * math.log2(math.e)
MESH = pl.DeviceIdType.MESH
SERVED, SPREAD = 0, 1
GATE_A, GATE_B = 2, 1


def kernel(
    n, order_hbm, exit_hbm, q_hbm, k_hbm, v_hbm, out_ref, live_hbm,
    qb, kv, acc, den, done, exits, order_ref, exit_ref, live_ref, kv_sem, q_sem,
    small_sem, send_sem, recv_sem, pair_send, pair_recv, exit_send, exit_recv, ready,
):
    me = lax.axis_index("seq")
    core = lax.axis_index("head")
    tiles = kv.shape[2]
    heads, rows = qb.shape[1:3]
    q_half = heads * HD
    far = n - 1
    at_end = (me == 0) | (me == far)
    serves = (me == 1) | (me == far - 1)
    end = jnp.where(me < n // 2, 0, far)
    inward = jnp.where(me < n // 2, 1, -1)
    first = core

    def inside(owner):
        return (owner >= 0) & (owner < n)

    def peer(step):
        return {"seq": jnp.clip(me + step, 0, far)}

    def own_copy(hh, which):
        src = (k_hbm, v_hbm)[which]
        return pltpu.make_async_copy(
            src.at[:, :, pl.ds(pl.multiple_of(hh * HD, HD), HD)],
            kv.at[me, hh, :, which],
            kv_sem.at[hh, which],
        )

    def own_queries(hh, h):
        return pltpu.make_async_copy(
            q_hbm.at[:, pl.ds(hh * q_half + h * HD, HD)], qb.at[hh, h], q_sem.at[hh, h]
        )

    small = [
        pltpu.make_async_copy(exit_hbm, exit_ref, small_sem.at[0]),
        pltpu.make_async_copy(order_hbm, order_ref, small_sem.at[1]),
    ]
    result = pltpu.make_async_copy(live_ref, live_hbm, small_sem.at[2])

    barrier = pltpu.get_barrier_semaphore()

    @pl.when(inside(me + 1))
    def _():
        pl.semaphore_signal(barrier, inc=1, device_id=peer(1), device_id_type=MESH)

    small[0].start()
    for which in range(2):
        own_copy(first, which).start()
    for h in range(heads):
        own_queries(0, h).start()
    small[1].start()
    for which in range(2):
        own_copy(1 - first, which).start()
    for h in range(heads):
        own_queries(1, h).start()

    small[0].wait()
    lane = lax.broadcasted_iota(jnp.int32, (1, TILE), 1)
    mine = jnp.zeros((1, TILE), jnp.int32)
    for i in range(tiles):
        mine = jnp.where(lane == i, exit_ref[i], mine)
    exits[me] = mine

    @pl.when(inside(me - 1))
    def _():
        pl.semaphore_wait(barrier, 1)
        pl.semaphore_signal(ready, inc=1, device_id=peer(-1), device_id_type=MESH)

    def hop(owner, hh, t, step):
        return pltpu.make_async_remote_copy(
            src_ref=kv.at[owner, hh, t],
            dst_ref=kv.at[owner, hh, t],
            send_sem=send_sem.at[jnp.where((owner == me) & (step < 0), n, owner), hh, t],
            recv_sem=recv_sem.at[owner, hh, t],
            device_id=peer(step),
            device_id_type=MESH,
        )

    def exit_hop(owner, step):
        return pltpu.make_async_remote_copy(
            src_ref=exits.at[owner],
            dst_ref=exits.at[owner],
            send_sem=exit_send.at[jnp.where((owner == me) & (step < 0), n, owner)],
            recv_sem=exit_recv.at[owner],
            device_id=peer(step),
            device_id_type=MESH,
        )

    def goes(hh, step):
        room = jnp.where(step > 0, far - me, me)
        return (room > 1) | ((room == 1) & (hh == SPREAD))

    def send(owner, hh, t, step):
        @pl.when(goes(hh, step))
        def _():
            hop(owner, hh, t, step).start()

    def send_own(hh, step):
        @pl.loop(0, tiles)
        def _(t):
            send(me, hh, t, step)

    def query_copy():
        return pltpu.make_async_remote_copy(
            src_ref=qb.at[0], dst_ref=qb.at[2],
            send_sem=pair_send.at[tiles], recv_sem=pair_recv.at[tiles],
            device_id=peer(inward), device_id_type=MESH,
        )

    def done_copy(t):
        part = pl.ds(t * TILE, TILE)
        return pltpu.make_async_remote_copy(
            src_ref=done.at[0, part], dst_ref=done.at[1, part],
            send_sem=pair_send.at[t], recv_sem=pair_recv.at[t],
            device_id=peer(-inward), device_id_type=MESH,
        )

    def wait_own(hh):
        for which in range(2):
            own_copy(hh, which).wait()

    def open_side(step):
        exit_hop(me, step).start()

        @pl.when(~at_end)
        def _():
            send_own(first, step)

        @pl.when(at_end & (core == 0))
        def _():
            query_copy().start()
            send_own(SERVED, step)

    wait_own(first)
    for h in range(heads):
        own_queries(0, h).wait()

    @pl.when(inside(me - 1))
    def _():
        open_side(-1)

    @pl.when(inside(me + 1))
    def _():
        pl.semaphore_wait(ready, 1)
        open_side(1)

    wait_own(1 - first)

    @pl.when(~at_end)
    def _():
        send_own(1 - first, -inward)

        @pl.when(core == 1)
        def _():
            send_own(SERVED, inward)

    acc[...] = jnp.zeros_like(acc)
    den[...] = jnp.zeros_like(den)

    for h in range(heads):
        own_queries(1, h).wait()
    small[1].wait()
    ahead = lax.broadcasted_iota(jnp.int32, (TILE, TILE), 1) - lax.broadcasted_iota(
        jnp.int32, (TILE, TILE), 0
    )

    def fold_into(slot, row_owner, owner, hh, t):
        key_place = order_ref[owner * tiles + t]
        over = jnp.stack(
            [
                ahead - (order_ref[row_owner * tiles + i] - key_place) * TILE
                for i in range(tiles)
            ]
        )
        stacked = (heads * rows, HD)
        scores = lax.dot_general(
            qb[slot].reshape(stacked), kv[owner, hh, t, 0],
            (((1,), (1,)), ((), ())), preferred_element_type=jnp.float32,
        ).reshape(heads, tiles, TILE, TILE)
        weights = jnp.where(
            over[None] <= 0, jnp.exp2(OUT_SCALE * jnp.tanh(scores * IN_SCALE)), 0.0
        ).reshape(heads * rows, TILE)
        den[slot] += weights
        acc[slot] += jnp.dot(
            weights.astype(jnp.bfloat16), kv[owner, hh, t, 1],
            preferred_element_type=jnp.float32,
        )

    def finish(slot, i, h):
        here = pl.ds(h * rows + i * TILE, TILE)
        total = jnp.sum(den[slot, here, :], axis=1, keepdims=True)
        return (acc[slot, here, :] / total).astype(jnp.bfloat16)

    def live_only(i, rows_out):
        return jnp.where(exit_ref[i] > 0, rows_out, jnp.zeros_like(rows_out))

    def keep(slot, i, h):
        out_ref[pl.ds(i * TILE, TILE), pl.ds(slot * q_half + h * HD, HD)] = live_only(
            i, finish(slot, i, h)
        )

    @pl.loop(jnp.where(at_end, tiles * (1 - core), 0), jnp.where(at_end, tiles * (2 - core), 2 * tiles))
    def _(k):
        hh = jnp.where(k < tiles, first, 1 - first)
        fold_into(hh, me, me, hh, lax.rem(k, tiles))

    def arrive(owner, hh, t, side):
        hop(owner, hh, t, side).wait_recv()
        send(owner, hh, t, -side)

        @pl.when((hh == SPREAD) & (t == 0))
        def _():
            exit_hop(owner, side).wait_recv()

            @pl.when(inside(me - side))
            def _():
                exit_hop(owner, -side).start()

    early = core == 0

    @pl.loop(0, 2 * far)
    def _(u):
        hh_in = jnp.where(early, u >= far, (u == 0) | (u > far)).astype(jnp.int32)
        s_in = jnp.where(
            u >= far + 1 - early, u - far + 1, jnp.where(early, u + 1, jnp.maximum(u, 1))
        )
        hh_out = (u >= far).astype(jnp.int32)
        s_out = jnp.where(u >= far, u - far + 1, u + early)
        from_in = me + inward * s_in
        from_out = me - inward * s_out
        has_in = inside(from_in) & ~(at_end & (hh_in == SERVED))
        has_out = inside(from_out) & (s_out > 0) & ~at_end
        serving = serves & (hh_in == SERVED) & inside(from_in)

        @pl.when(has_in | has_out)
        def _():
            @pl.loop(0, tiles)
            def _(t):
                @pl.when((u == 2 * far - 1) & (t == tiles - 1) & at_end)
                def _():
                    for i in range(tiles):
                        here = pl.ds(i * TILE, TILE)
                        done_copy(i).wait_recv()
                        out_ref[here, pl.ds(0, q_half)] = live_only(i, done[1, here, :])

                @pl.when(has_in)
                def _():
                    arrive(from_in, hh_in, t, inward)

                @pl.when(has_out)
                def _():
                    arrive(from_out, hh_out, t, -inward)

                @pl.when(early & ~at_end & (u == 0) & (t == tiles - 1))
                def _():
                    send_own(SPREAD, inward)

                @pl.when(~early & at_end & (u == 0) & (t == GATE_B))
                def _():
                    query_copy().start()
                    send_own(SERVED, inward)
                    send_own(SPREAD, inward)

                @pl.when(early & at_end & (u == far) & (t == GATE_A))
                def _():
                    send_own(SPREAD, inward)

                @pl.when(serving & (s_in == 1) & (t == 0))
                def _():
                    query_copy().wait_recv()

                @pl.loop(jnp.where(has_in, 0, 1), jnp.where(serving, jnp.where(s_in == 1, 5, 3), jnp.where(has_out, 2, 1)))
                def _(k):
                    owner = jnp.where(k == 4, me, jnp.where((k == 1) | (k == 3), from_out, from_in))
                    hh = jnp.where(k == 1, hh_out, hh_in)

                    @pl.when(has_out | (k != 1))
                    def _():
                        fold_into(
                            jnp.where(k > 1, 2, hh), jnp.where(k > 1, end, me), owner, hh, t
                        )

        @pl.when(serving & (s_in == far - 1))
        def _():
            for t in range(tiles):
                for h in range(heads):
                    done[0, pl.ds(t * TILE, TILE), pl.ds(h * HD, HD)] = finish(2, t, h)
                if t > 0:
                    done_copy(t - 1).start()
            for h in range(heads):
                keep(0, 0, h)
            done_copy(tiles - 1).start()

    live_ref[0] = jnp.sum((exits[...] > 0).astype(jnp.int32))
    result.start()

    for i in range(tiles):
        for h in range(heads):
            keep(1, i, h)

    @pl.when(~at_end)
    def _():
        for i in range(tiles):
            for h in range(heads):
                keep(0, i, h)

    @pl.when(at_end)
    def _():
        query_copy().wait_send()

    @pl.when(serves)
    def _():
        for t in range(tiles):
            done_copy(t).wait_send()

    for step in (1, -1):
        @pl.loop(0, n)
        def _(s):
            owner = me - step * s

            @pl.when(inside(owner) & inside(me + step))
            def _():
                exit_hop(owner, step).wait_send()

            @pl.loop(0, 2)
            def _(hh):
                @pl.when(inside(owner) & goes(hh, step))
                def _():
                    @pl.loop(0, tiles)
                    def _(t):
                        hop(owner, hh, t, step).wait_send()

    result.wait()


def body(n, queries, keys, values, exit_layer, tile_order):
    rows, q_width = queries.shape[1:]
    kv_width = keys.shape[2]
    q_half = q_width // 2
    heads = q_half // HD
    tiles = rows // TILE
    hbm = pl.BlockSpec(memory_space=pltpu.HBM)
    vmem = pl.BlockSpec(memory_space=pltpu.VMEM)
    dma = pltpu.SemaphoreType.DMA
    attended, live = pl.pallas_call(
        functools.partial(kernel, n),
        out_shape=(
            pltpu.VMEM((rows, q_width), jnp.bfloat16),
            jax.ShapeDtypeStruct((1,), jnp.int32),
        ),
        in_specs=[hbm] * 5,
        out_specs=(vmem, hbm),
        scratch_shapes=[
            pltpu.VMEM((3, heads, rows, HD), jnp.bfloat16),
            pltpu.VMEM((n, 2, tiles, 2, TILE, HD), jnp.bfloat16),
            pltpu.VMEM((3, heads * rows, HD), jnp.float32),
            pltpu.VMEM((3, heads * rows, TILE), jnp.float32),
            pltpu.VMEM((2, rows, q_half), jnp.bfloat16),
            pltpu.VMEM((n, 1, TILE), jnp.int32),
            pltpu.SMEM(tile_order.shape, jnp.int32),
            pltpu.SMEM(exit_layer.shape, jnp.int32),
            pltpu.SMEM((1,), jnp.int32),
            dma((2, 2)),
            dma((2, heads)),
            dma((3,)),
            dma((n + 1, 2, tiles)),
            dma((n, 2, tiles)),
            dma((tiles + 1,)),
            dma((tiles + 1,)),
            dma((n + 1,)),
            dma((n,)),
            pltpu.SemaphoreType.REGULAR,
        ],
        compiler_params=pltpu.CompilerParams(
            collective_id=0, has_side_effects=True, vmem_limit_bytes=62_500_000
        ),
        name="attend_line",
    )(
        tile_order, exit_layer, queries[0],
        keys.reshape(tiles, TILE, kv_width), values.reshape(tiles, TILE, kv_width),
    )
    return attended[None], live


def solution(mesh):
    return jax.shard_map(
        functools.partial(body, mesh.shape["seq"]),
        mesh=mesh,
        in_specs=(
            P(None, ("batch", "seq"), "head"),
            P(None, ("batch", "seq"), "head"),
            P(None, ("batch", "seq"), "head"),
            P(("batch", "seq")),
            P("batch"),
        ),
        out_specs=(P(None, ("batch", "seq"), "head"), P("batch")),
        check_vma=False,
    )
```

```python
import functools
import math

import jax
import jax.numpy as jnp
from jax import lax
from jax.experimental import pallas as pl
from jax.experimental.pallas import tpu as pltpu
from jax.sharding import PartitionSpec as P

HD = 256
TILE = 128
SOFTCAP = 50.0
QUERY_SCALE = 0.0625
IN_SCALE = QUERY_SCALE / SOFTCAP
OUT_SCALE = SOFTCAP * math.log2(math.e)
MESH = pl.DeviceIdType.MESH
SERVED, SPREAD = 0, 1
GATE_A, GATE_B, AHEAD = 2, 2, 2


def kernel(
    n, order_hbm, exit_hbm, q_hbm, k_hbm, v_hbm, out_ref, live_hbm,
    qb, kv, acc, den, done, exits, order_ref, exit_ref, live_ref, kv_sem, q_sem,
    small_sem, send_sem, recv_sem, pair_send, pair_recv, exit_recv, ready,
):
    me = lax.axis_index("seq")
    core = lax.axis_index("head")
    tiles = kv.shape[2]
    heads, rows = qb.shape[1:3]
    q_half = heads * HD
    far = n - 1
    at_end = (me == 0) | (me == far)
    serves = (me == 1) | (me == far - 1)
    end = jnp.where(me < n // 2, 0, far)
    inward = jnp.where(me < n // 2, 1, -1)
    first = core

    def inside(owner):
        return (owner >= 0) & (owner < n)

    def peer(step):
        return {"seq": jnp.clip(me + step, 0, far)}

    def load_own(hh):
        for which, src in enumerate((k_hbm, v_hbm)):
            pltpu.make_async_copy(
                src.at[:, :, pl.ds(pl.multiple_of(hh * HD, HD), HD)],
                kv.at[me, hh, :, which],
                kv_sem.at[hh],
            ).start()

    def wait_own(hh):
        pltpu.make_async_copy(kv.at[me, hh], kv.at[me, hh], kv_sem.at[hh]).wait()

    def load_queries(hh):
        for h in range(heads):
            pltpu.make_async_copy(
                q_hbm.at[:, pl.ds(hh * q_half + h * HD, HD)], qb.at[hh, h], q_sem.at[hh]
            ).start()

    def wait_queries(hh):
        pltpu.make_async_copy(qb.at[hh], qb.at[hh], q_sem.at[hh]).wait()

    small = [
        pltpu.make_async_copy(exit_hbm, exit_ref, small_sem.at[0]),
        pltpu.make_async_copy(order_hbm, order_ref, small_sem.at[1]),
    ]
    result = pltpu.make_async_copy(live_ref, live_hbm, small_sem.at[2])

    barrier = pltpu.get_barrier_semaphore()

    @pl.when(inside(me + 1))
    def _():
        pl.semaphore_signal(barrier, inc=1, device_id=peer(1), device_id_type=MESH)

    small[0].start()
    load_own(first)
    asks = at_end & (core == 0)

    @pl.when(asks)
    def _():
        load_queries(0)

    small[0].wait()
    lane = lax.broadcasted_iota(jnp.int32, (1, TILE), 1)
    mine = jnp.zeros((1, TILE), jnp.int32)
    for i in range(tiles):
        mine = jnp.where(lane == i, exit_ref[i], mine)
    exits[me] = mine

    @pl.when(inside(me - 1))
    def _():
        pl.semaphore_wait(barrier, 1)
        pl.semaphore_signal(ready, inc=1, device_id=peer(-1), device_id_type=MESH)

    soon = min(AHEAD, tiles - 1)

    def hop(owner, hh, t, step):
        return pltpu.make_async_remote_copy(
            src_ref=kv.at[owner, hh, t],
            dst_ref=kv.at[owner, hh, t],
            send_sem=send_sem.at[0, jnp.where(step > 0, 1, 0)],
            recv_sem=recv_sem.at[owner, hh, t],
            device_id=peer(step),
            device_id_type=MESH,
        )

    def exit_hop(owner, step):
        return pltpu.make_async_remote_copy(
            src_ref=exits.at[owner],
            dst_ref=exits.at[owner],
            send_sem=send_sem.at[1, jnp.where(step > 0, 1, 0)],
            recv_sem=exit_recv.at[owner],
            device_id=peer(step),
            device_id_type=MESH,
        )

    def goes(hh, step):
        room = jnp.where(step > 0, far - me, me)
        return (room > 1) | ((room == 1) & (hh == SPREAD))

    def send(owner, hh, t, step):
        @pl.when(goes(hh, step))
        def _():
            hop(owner, hh, t, step).start()

    def send_own(hh, step, low=0, high=tiles):
        @pl.loop(low, high)
        def _(t):
            send(me, hh, t, step)

    def query_copy():
        return pltpu.make_async_remote_copy(
            src_ref=qb.at[0], dst_ref=qb.at[2],
            send_sem=pair_send.at[0], recv_sem=pair_recv.at[0],
            device_id=peer(inward), device_id_type=MESH,
        )

    def done_copy(low, count, last):
        part = pl.ds(low * TILE, count * TILE)
        return pltpu.make_async_remote_copy(
            src_ref=done.at[0, part], dst_ref=done.at[1, part],
            send_sem=pair_send.at[1], recv_sem=pair_recv.at[2 if last else 1],
            device_id=peer(-inward), device_id_type=MESH,
        )

    def open_side(step):
        exit_hop(me, step).start()

        @pl.when(~at_end)
        def _():
            send_own(first, step)

        @pl.when(at_end & (core == 0))
        def _():
            query_copy().start()
            send_own(SERVED, step)

        @pl.when(at_end & (core == 1))
        def _():
            send_own(SPREAD, step, 0, soon)

    @pl.when(asks)
    def _():
        wait_queries(0)

    wait_own(first)

    @pl.when(inside(me - 1))
    def _():
        open_side(-1)

    @pl.when(inside(me + 1))
    def _():
        pl.semaphore_wait(ready, 1)
        open_side(1)

    load_own(1 - first)
    load_queries(1)
    small[1].start()

    @pl.when(~asks)
    def _():
        load_queries(0)

    wait_own(1 - first)

    @pl.when(~at_end)
    def _():
        send_own(1 - first, -inward)

    acc[...] = jnp.zeros_like(acc)
    den[...] = jnp.zeros_like(den)

    @pl.when(~asks)
    def _():
        wait_queries(0)

    wait_queries(1)
    small[1].wait()
    ahead = lax.broadcasted_iota(jnp.int32, (TILE, TILE), 1) - lax.broadcasted_iota(
        jnp.int32, (TILE, TILE), 0
    )

    def fold_into(slot, row_owner, owner, hh, t):
        key_place = order_ref[owner * tiles + t]
        over = jnp.stack(
            [
                ahead - (order_ref[row_owner * tiles + i] - key_place) * TILE
                for i in range(tiles)
            ]
        )
        stacked = (heads * rows, HD)
        scores = lax.dot_general(
            qb[slot].reshape(stacked), kv[owner, hh, t, 0],
            (((1,), (1,)), ((), ())), preferred_element_type=jnp.float32,
        ).reshape(heads, tiles, TILE, TILE)
        weights = jnp.where(
            over[None] <= 0, jnp.exp2(OUT_SCALE * jnp.tanh(scores * IN_SCALE)), 0.0
        ).reshape(heads * rows, TILE)
        den[slot] += weights
        acc[slot] += jnp.dot(
            weights.astype(jnp.bfloat16), kv[owner, hh, t, 1],
            preferred_element_type=jnp.float32,
        )

    def finish(slot, i, h):
        here = pl.ds(h * rows + i * TILE, TILE)
        total = jnp.sum(den[slot, here, :], axis=1, keepdims=True)
        return (acc[slot, here, :] / total).astype(jnp.bfloat16)

    def live_only(i, rows_out):
        return jnp.where(exit_ref[i] > 0, rows_out, jnp.zeros_like(rows_out))

    def keep(slot, i, h):
        out_ref[pl.ds(i * TILE, TILE), pl.ds(slot * q_half + h * HD, HD)] = live_only(
            i, finish(slot, i, h)
        )

    @pl.loop(jnp.where(at_end, tiles * (1 - core), 0), jnp.where(at_end, tiles * (2 - core), 2 * tiles))
    def _(k):
        hh = jnp.where(k < tiles, first, 1 - first)
        fold_into(hh, me, me, hh, lax.rem(k, tiles))

    def arrive(owner, hh, t, side):
        hop(owner, hh, t, side).wait_recv()
        send(owner, hh, t, -side)

        @pl.when((hh == SPREAD) & (t == 0))
        def _():
            exit_hop(owner, side).wait_recv()

            @pl.when(inside(me - side))
            def _():
                exit_hop(owner, -side).start()

    def collect(i):
        here = pl.ds(i * TILE, TILE)
        out_ref[here, pl.ds(0, q_half)] = live_only(i, done[1, here, :])

    early = core == 0

    @pl.loop(0, 3 * far - 1)
    def _(u):
        spread_a = u >= far
        s_a = jnp.where(spread_a, u - far + 1, u + 1)
        served_b = (u >= far) & (u < 2 * far)
        late_b = u >= 2 * far
        s_b = jnp.where(late_b, u - 2 * far + 2, jnp.where(served_b, u - far + 1, u + 1))
        hh_in = jnp.where(early, spread_a, ~served_b).astype(jnp.int32)
        s_in = jnp.where(early, s_a, s_b)
        extra = serves & (u == far + 1)
        hh_out = jnp.where(early, spread_a, ~served_b | extra).astype(jnp.int32)
        s_out = jnp.where(early, s_a, jnp.where(extra, 1, jnp.where(late_b, s_b - 1, s_b)))
        part_in = ~early & (u > 0) & (hh_in == SPREAD)
        low_in = jnp.where(part_in & late_b, soon, 0)
        high_in = jnp.where(part_in & ~late_b, soon, tiles)
        part_out = ~early & (hh_out == SPREAD)
        low_out = jnp.where(part_out & (late_b | extra), soon, 0)
        high_out = jnp.where(part_out & ~(late_b | extra), soon, tiles)
        from_in = me + inward * s_in
        from_out = me - inward * s_out
        runs = ~early | (u < 2 * far)
        any_in = runs & inside(from_in) & ~(at_end & (hh_in == SERVED))
        any_out = runs & inside(from_out) & ~at_end & ~(late_b & ~early & serves)
        serving = runs & serves & (hh_in == SERVED) & inside(from_in)

        @pl.when(any_in | any_out)
        def _():
            @pl.loop(0, tiles)
            def _(t):
                has_in = any_in & (t >= low_in) & (t < high_in)
                has_out = any_out & (t >= low_out) & (t < high_out)

                @pl.when((u == jnp.where(early, 2 * far - 1, 3 * far - 2)) & (t == tiles - 1) & at_end)
                def _():
                    done_copy(0, tiles - 1, False).wait_recv()
                    for i in range(tiles - 1):
                        collect(i)

                @pl.when(has_out)
                def _():
                    arrive(from_out, hh_out, t, -inward)

                @pl.when(has_in)
                def _():
                    arrive(from_in, hh_in, t, inward)

                @pl.when(~early & serves & (u == 2 * far) & (t == tiles - 1))
                def _():
                    done_copy(tiles - 1, 1, True).start()

                @pl.when(early & ~at_end & (u == 0) & (t == tiles - 1))
                def _():
                    send_own(SPREAD, inward)

                @pl.when(~early & ~at_end & (u == 0) & (t == soon - 1))
                def _():
                    send_own(SERVED, inward)

                @pl.when(~early & at_end & (u == 0) & (t == GATE_B))
                def _():
                    query_copy().start()
                    send_own(SERVED, inward)
                    send_own(SPREAD, inward, soon, tiles)

                @pl.when(early & at_end & (u == far) & (t == GATE_A))
                def _():
                    send_own(SPREAD, inward)

                @pl.when(serving & (s_in == 1) & (t == 0))
                def _():
                    query_copy().wait_recv()

                @pl.loop(jnp.where(serving, 0, 3), jnp.where(has_out, 5, 4))
                def _(k):
                    owner = jnp.where(
                        k == 2, me, jnp.where((k == 1) | (k == 4), from_out, from_in)
                    )

                    @pl.when(jnp.where((k == 1) | (k == 2), s_in == 1, (k != 3) | has_in))
                    def _():
                        hh = jnp.where(k == 4, hh_out, hh_in)
                        fold_into(
                            jnp.where(k < 3, 2, hh), jnp.where(k < 3, end, me), owner, hh, t
                        )

        @pl.when(serving & (s_in == far - 1))
        def _():
            for t in range(tiles):
                for h in range(heads):
                    done[0, pl.ds(t * TILE, TILE), pl.ds(h * HD, HD)] = finish(2, t, h)
                if t > 0:
                    done_copy(t - 1, 1, False).start()

            @pl.when(early)
            def _():
                for h in range(heads):
                    keep(0, 0, h)
                done_copy(tiles - 1, 1, True).start()

    live_ref[0] = jnp.sum((exits[...] > 0).astype(jnp.int32))
    result.start()

    for i in range(tiles):
        for h in range(heads):
            keep(1, i, h)

    @pl.when(~at_end)
    def _():
        for i in range(tiles):
            for h in range(heads):
                keep(0, i, h)

    @pl.when(at_end)
    def _():
        done_copy(tiles - 1, 1, True).wait_recv()
        collect(tiles - 1)
        query_copy().wait_send()

    @pl.when(serves)
    def _():
        done_copy(0, tiles, True).wait_send()

    for step in (1, -1):
        room = jnp.where(step > 0, far - me, me)
        count = n - room

        def sent(ref, row):
            return pltpu.make_async_remote_copy(
                src_ref=ref, dst_ref=ref,
                send_sem=send_sem.at[row, (step + 1) // 2], recv_sem=exit_recv.at[0],
                device_id=peer(step), device_id_type=MESH,
            )

        @pl.when(room == 1)
        def _():
            sent(kv.at[pl.ds(0, far), SPREAD], 0).wait_send()

        for c in range(1, n):
            @pl.when(count == c)
            def _():
                sent(exits.at[pl.ds(0, c)], 1).wait_send()

            if c < far:
                @pl.when(count == c)
                def _():
                    sent(kv.at[pl.ds(0, c)], 0).wait_send()

    result.wait()


def body(n, queries, keys, values, exit_layer, tile_order):
    rows, q_width = queries.shape[1:]
    kv_width = keys.shape[2]
    q_half = q_width // 2
    heads = q_half // HD
    tiles = rows // TILE
    hbm = pl.BlockSpec(memory_space=pltpu.HBM)
    vmem = pl.BlockSpec(memory_space=pltpu.VMEM)
    dma = pltpu.SemaphoreType.DMA
    attended, live = pl.pallas_call(
        functools.partial(kernel, n),
        out_shape=(
            pltpu.VMEM((rows, q_width), jnp.bfloat16),
            jax.ShapeDtypeStruct((1,), jnp.int32),
        ),
        in_specs=[hbm] * 5,
        out_specs=(vmem, hbm),
        scratch_shapes=[
            pltpu.VMEM((3, heads, rows, HD), jnp.bfloat16),
            pltpu.VMEM((n, 2, tiles, 2, TILE, HD), jnp.bfloat16),
            pltpu.VMEM((3, heads * rows, HD), jnp.float32),
            pltpu.VMEM((3, heads * rows, TILE), jnp.float32),
            pltpu.VMEM((2, rows, q_half), jnp.bfloat16),
            pltpu.VMEM((n, 1, TILE), jnp.int32),
            pltpu.SMEM(tile_order.shape, jnp.int32),
            pltpu.SMEM(exit_layer.shape, jnp.int32),
            pltpu.SMEM((1,), jnp.int32),
            dma((2,)),
            dma((2,)),
            dma((3,)),
            dma((2, 2)),
            dma((n, 2, tiles)),
            dma((2,)),
            dma((3,)),
            dma((n,)),
            pltpu.SemaphoreType.REGULAR,
        ],
        compiler_params=pltpu.CompilerParams(
            collective_id=0, has_side_effects=True, vmem_limit_bytes=62_500_000
        ),
        name="attend_line",
    )(
        tile_order, exit_layer, queries[0],
        keys.reshape(tiles, TILE, kv_width), values.reshape(tiles, TILE, kv_width),
    )
    return attended[None], live


def solution(mesh):
    return jax.shard_map(
        functools.partial(body, mesh.shape["seq"]),
        mesh=mesh,
        in_specs=(
            P(None, ("batch", "seq"), "head"),
            P(None, ("batch", "seq"), "head"),
            P(None, ("batch", "seq"), "head"),
            P(("batch", "seq")),
            P("batch"),
        ),
        out_specs=(P(None, ("batch", "seq"), "head"), P("batch")),
        check_vma=False,
    )
```

```python
import functools
import math

import jax
import jax.numpy as jnp
from jax import lax
from jax.experimental import pallas as pl
from jax.experimental.pallas import tpu as pltpu
from jax.sharding import PartitionSpec as P

HD = 256
TILE = 128
SOFTCAP = 50.0
QUERY_SCALE = 0.0625
IN_SCALE = QUERY_SCALE / SOFTCAP
OUT_SCALE = SOFTCAP * math.log2(math.e)
MESH = pl.DeviceIdType.MESH
SERVED, SPREAD = 0, 1
GATE_A, GATE_B, AHEAD = 2, 2, 1


def kernel(
    n, order_hbm, exit_hbm, q_hbm, k_hbm, v_hbm, out_ref, live_hbm,
    qb, kv, acc, den, done, exits, order_ref, exit_ref, live_ref, kv_sem, q_sem,
    small_sem, send_sem, recv_sem, pair_send, pair_recv, exit_recv, ready,
):
    me = lax.axis_index("seq")
    core = lax.axis_index("head")
    tiles = kv.shape[2]
    heads, rows = qb.shape[1:3]
    q_half = heads * HD
    far = n - 1
    at_end = (me == 0) | (me == far)
    serves = (me == 1) | (me == far - 1)
    end = jnp.where(me < n // 2, 0, far)
    inward = jnp.where(me < n // 2, 1, -1)
    first = core

    def inside(owner):
        return (owner >= 0) & (owner < n)

    def peer(step):
        return {"seq": jnp.clip(me + step, 0, far)}

    def load_own(hh):
        for which, src in enumerate((k_hbm, v_hbm)):
            pltpu.make_async_copy(
                src.at[:, :, pl.ds(pl.multiple_of(hh * HD, HD), HD)],
                kv.at[me, hh, :, which],
                kv_sem.at[hh],
            ).start()

    def wait_own(hh):
        pltpu.make_async_copy(kv.at[me, hh], kv.at[me, hh], kv_sem.at[hh]).wait()

    def load_queries(hh):
        for h in range(heads):
            pltpu.make_async_copy(
                q_hbm.at[:, pl.ds(hh * q_half + h * HD, HD)], qb.at[hh, h], q_sem.at[hh]
            ).start()

    def wait_queries(hh):
        pltpu.make_async_copy(qb.at[hh], qb.at[hh], q_sem.at[hh]).wait()

    small = [
        pltpu.make_async_copy(exit_hbm, exit_ref, small_sem.at[0]),
        pltpu.make_async_copy(order_hbm, order_ref, small_sem.at[1]),
    ]
    result = pltpu.make_async_copy(live_ref, live_hbm, small_sem.at[2])

    barrier = pltpu.get_barrier_semaphore()

    @pl.when(inside(me + 1))
    def _():
        pl.semaphore_signal(barrier, inc=1, device_id=peer(1), device_id_type=MESH)

    small[0].start()
    load_own(first)
    asks = at_end & (core == 0)

    @pl.when(asks)
    def _():
        load_queries(0)

    small[0].wait()
    lane = lax.broadcasted_iota(jnp.int32, (1, TILE), 1)
    mine = jnp.zeros((1, TILE), jnp.int32)
    for i in range(tiles):
        mine = jnp.where(lane == i, exit_ref[i], mine)
    exits[me] = mine

    @pl.when(inside(me - 1))
    def _():
        pl.semaphore_wait(barrier, 1)
        pl.semaphore_signal(ready, inc=1, device_id=peer(-1), device_id_type=MESH)

    soon = min(AHEAD, tiles - 1)

    def hop(owner, hh, t, step):
        return pltpu.make_async_remote_copy(
            src_ref=kv.at[owner, hh, t],
            dst_ref=kv.at[owner, hh, t],
            send_sem=send_sem.at[0, jnp.where(step > 0, 1, 0)],
            recv_sem=recv_sem.at[owner, hh, t],
            device_id=peer(step),
            device_id_type=MESH,
        )

    def exit_hop(owner, step):
        return pltpu.make_async_remote_copy(
            src_ref=exits.at[owner],
            dst_ref=exits.at[owner],
            send_sem=send_sem.at[1, jnp.where(step > 0, 1, 0)],
            recv_sem=exit_recv.at[owner],
            device_id=peer(step),
            device_id_type=MESH,
        )

    def goes(hh, step):
        room = jnp.where(step > 0, far - me, me)
        return (room > 1) | ((room == 1) & (hh == SPREAD))

    def send(owner, hh, t, step):
        @pl.when(goes(hh, step))
        def _():
            hop(owner, hh, t, step).start()

    def send_own(hh, step, low=0, high=tiles):
        @pl.loop(low, high)
        def _(t):
            send(me, hh, t, step)

    def query_copy():
        return pltpu.make_async_remote_copy(
            src_ref=qb.at[0], dst_ref=qb.at[2],
            send_sem=pair_send.at[0], recv_sem=pair_recv.at[0],
            device_id=peer(inward), device_id_type=MESH,
        )

    def done_copy(low, count, last):
        part = pl.ds(low * TILE, count * TILE)
        return pltpu.make_async_remote_copy(
            src_ref=done.at[0, part], dst_ref=done.at[1, part],
            send_sem=pair_send.at[1], recv_sem=pair_recv.at[2 if last else 1],
            device_id=peer(-inward), device_id_type=MESH,
        )

    def open_side(step):
        exit_hop(me, step).start()

        @pl.when(~at_end)
        def _():
            send_own(first, step)

        @pl.when(at_end & (core == 0))
        def _():
            query_copy().start()
            send_own(SERVED, step)

        @pl.when(at_end & (core == 1))
        def _():
            send_own(SPREAD, step, 0, soon)

    @pl.when(asks)
    def _():
        wait_queries(0)

    wait_own(first)

    @pl.when(inside(me - 1))
    def _():
        open_side(-1)

    @pl.when(inside(me + 1))
    def _():
        pl.semaphore_wait(ready, 1)
        open_side(1)

    load_own(1 - first)
    load_queries(1)
    small[1].start()

    @pl.when(~asks)
    def _():
        load_queries(0)

    wait_own(1 - first)

    @pl.when(~at_end)
    def _():
        send_own(1 - first, -inward)

    acc[...] = jnp.zeros_like(acc)
    den[...] = jnp.zeros_like(den)

    @pl.when(~asks)
    def _():
        wait_queries(0)

    wait_queries(1)
    small[1].wait()
    ahead = lax.broadcasted_iota(jnp.int32, (TILE, TILE), 1) - lax.broadcasted_iota(
        jnp.int32, (TILE, TILE), 0
    )

    def fold_into(slot, row_owner, owner, hh, t):
        key_place = order_ref[owner * tiles + t]
        over = jnp.stack(
            [
                ahead - (order_ref[row_owner * tiles + i] - key_place) * TILE
                for i in range(tiles)
            ]
        )
        stacked = (heads * rows, HD)
        scores = lax.dot_general(
            qb[slot].reshape(stacked), kv[owner, hh, t, 0],
            (((1,), (1,)), ((), ())), preferred_element_type=jnp.float32,
        ).reshape(heads, tiles, TILE, TILE)
        weights = jnp.where(
            over[None] <= 0, jnp.exp2(OUT_SCALE * jnp.tanh(scores * IN_SCALE)), 0.0
        ).reshape(heads * rows, TILE)
        den[slot] += weights
        acc[slot] += jnp.dot(
            weights.astype(jnp.bfloat16), kv[owner, hh, t, 1],
            preferred_element_type=jnp.float32,
        )

    def finish(slot, i, h):
        here = pl.ds(h * rows + i * TILE, TILE)
        total = jnp.sum(den[slot, here, :], axis=1, keepdims=True)
        return (acc[slot, here, :] / total).astype(jnp.bfloat16)

    def live_only(i, rows_out):
        return jnp.where(exit_ref[i] > 0, rows_out, jnp.zeros_like(rows_out))

    def keep(slot, i, h):
        out_ref[pl.ds(i * TILE, TILE), pl.ds(slot * q_half + h * HD, HD)] = live_only(
            i, finish(slot, i, h)
        )

    @pl.loop(jnp.where(at_end, tiles * (1 - core), 0), jnp.where(at_end, tiles * (2 - core), 2 * tiles))
    def _(k):
        hh = jnp.where(k < tiles, first, 1 - first)
        fold_into(hh, me, me, hh, lax.rem(k, tiles))

    def arrive(owner, hh, t, side):
        hop(owner, hh, t, side).wait_recv()
        send(owner, hh, t, -side)

        @pl.when((hh == SPREAD) & (t == 0))
        def _():
            exit_hop(owner, side).wait_recv()

            @pl.when(inside(me - side))
            def _():
                exit_hop(owner, -side).start()

    def collect(i):
        here = pl.ds(i * TILE, TILE)
        out_ref[here, pl.ds(0, q_half)] = live_only(i, done[1, here, :])

    def finish_served():
        for t in range(tiles):
            for h in range(heads):
                done[0, pl.ds(t * TILE, TILE), pl.ds(h * HD, HD)] = finish(2, t, h)
            if t > 0:
                done_copy(t - 1, 1, False).start()

        @pl.when(core == 0)
        def _():
            for h in range(heads):
                keep(0, 0, h)
            done_copy(tiles - 1, 1, True).start()

    early = core == 0

    @pl.loop(0, 3 * far - 1)
    def _(u):
        spread_a = u >= far
        s_a = jnp.where(spread_a, u - far + 1, u + 1)
        served_b = (u >= far) & (u < 2 * far)
        late_b = u >= 2 * far
        s_b = jnp.where(late_b, u - 2 * far + 2, jnp.where(served_b, u - far + 1, u + 1))
        hh_in = jnp.where(early, spread_a, ~served_b).astype(jnp.int32)
        s_in = jnp.where(early, s_a, s_b)
        extra = serves & (u == far + 1)
        hh_out = jnp.where(early, spread_a, ~served_b | extra).astype(jnp.int32)
        s_out = jnp.where(early, s_a, jnp.where(extra, 1, jnp.where(late_b, s_b - 1, s_b)))
        part_in = ~early & (u > 0) & (hh_in == SPREAD)
        low_in = jnp.where(part_in & late_b, soon, 0)
        high_in = jnp.where(part_in & ~late_b, soon, tiles)
        part_out = ~early & (hh_out == SPREAD)
        low_out = jnp.where(part_out & (late_b | extra), soon, 0)
        high_out = jnp.where(part_out & ~(late_b | extra), soon, tiles)
        from_in = me + inward * s_in
        from_out = me - inward * s_out
        runs = ~early | (u < 2 * far)
        any_in = runs & inside(from_in) & ~(at_end & (hh_in == SERVED))
        any_out = runs & inside(from_out) & ~at_end & ~(late_b & ~early & serves)
        later = early & ~at_end & (hh_in == SERVED)
        both = early & ~at_end & (hh_in == SPREAD)
        serving = runs & serves & (hh_in == SERVED) & inside(from_in)

        @pl.when(any_in | any_out)
        def _():
            @pl.loop(0, tiles)
            def _(t):
                has_in = any_in & (t >= low_in) & (t < high_in)
                has_out = any_out & (t >= low_out) & (t < high_out)

                @pl.when((u == jnp.where(early, 2 * far - 1, 3 * far - 2)) & (t == tiles - 1) & at_end)
                def _():
                    done_copy(0, tiles - 1, False).wait_recv()
                    for i in range(tiles - 1):
                        collect(i)

                @pl.when(has_out)
                def _():
                    arrive(from_out, hh_out, t, -inward)

                @pl.when(has_in)
                def _():
                    arrive(from_in, hh_in, t, inward)

                @pl.when(~early & serves & (u == 2 * far) & (t == tiles - 1))
                def _():
                    done_copy(tiles - 1, 1, True).start()

                @pl.when(early & ~at_end & (u == 0) & (t == tiles - 1))
                def _():
                    send_own(SPREAD, inward)

                @pl.when(~early & ~at_end & (u == 0) & (t == soon - 1))
                def _():
                    send_own(SERVED, inward)

                @pl.when(~early & at_end & (u == 0) & (t == GATE_B))
                def _():
                    query_copy().start()
                    send_own(SERVED, inward)
                    send_own(SPREAD, inward, soon, tiles)

                @pl.when(early & at_end & (u == far) & (t == GATE_A))
                def _():
                    send_own(SPREAD, inward)

                @pl.when(serving & (s_in == 1) & (t == 0))
                def _():
                    query_copy().wait_recv()

                @pl.loop(0, jnp.where(serving, jnp.where(s_in == 1, 3, 1), 0))
                def _(k):
                    owner = jnp.where(k == 2, me, jnp.where(k == 1, from_out, from_in))
                    fold_into(2, end, owner, SERVED, t)

                @pl.when(serving & (s_in == far - 1) & (t == tiles - 1))
                def _():
                    finish_served()

                @pl.loop(jnp.where(has_in, 0, 1), jnp.where(both, 4, 2))
                def _(k):
                    outer = (k % 2) == 1

                    @pl.when(jnp.where(outer, has_out, has_in) & ~later)
                    def _():
                        hh = jnp.where(k > 1, SERVED, jnp.where(outer, hh_out, hh_in))
                        fold_into(hh, me, jnp.where(outer, from_out, from_in), hh, t)

    live_ref[0] = jnp.sum((exits[...] > 0).astype(jnp.int32))
    result.start()

    for i in range(tiles):
        for h in range(heads):
            keep(1, i, h)

    @pl.when(~at_end)
    def _():
        for i in range(tiles):
            for h in range(heads):
                keep(0, i, h)

    @pl.when(at_end)
    def _():
        done_copy(tiles - 1, 1, True).wait_recv()
        collect(tiles - 1)
        query_copy().wait_send()

    @pl.when(serves)
    def _():
        done_copy(0, tiles, True).wait_send()

    for step in (1, -1):
        room = jnp.where(step > 0, far - me, me)
        count = n - room

        def sent(ref, row):
            return pltpu.make_async_remote_copy(
                src_ref=ref, dst_ref=ref,
                send_sem=send_sem.at[row, (step + 1) // 2], recv_sem=exit_recv.at[0],
                device_id=peer(step), device_id_type=MESH,
            )

        @pl.when(room == 1)
        def _():
            sent(kv.at[pl.ds(0, far), SPREAD], 0).wait_send()

        for c in range(1, n):
            @pl.when(count == c)
            def _():
                sent(exits.at[pl.ds(0, c)], 1).wait_send()

            if c < far:
                @pl.when(count == c)
                def _():
                    sent(kv.at[pl.ds(0, c)], 0).wait_send()

    result.wait()


def body(n, queries, keys, values, exit_layer, tile_order):
    rows, q_width = queries.shape[1:]
    kv_width = keys.shape[2]
    q_half = q_width // 2
    heads = q_half // HD
    tiles = rows // TILE
    hbm = pl.BlockSpec(memory_space=pltpu.HBM)
    vmem = pl.BlockSpec(memory_space=pltpu.VMEM)
    dma = pltpu.SemaphoreType.DMA
    attended, live = pl.pallas_call(
        functools.partial(kernel, n),
        out_shape=(
            pltpu.VMEM((rows, q_width), jnp.bfloat16),
            jax.ShapeDtypeStruct((1,), jnp.int32),
        ),
        in_specs=[hbm] * 5,
        out_specs=(vmem, hbm),
        scratch_shapes=[
            pltpu.VMEM((3, heads, rows, HD), jnp.bfloat16),
            pltpu.VMEM((n, 2, tiles, 2, TILE, HD), jnp.bfloat16),
            pltpu.VMEM((3, heads * rows, HD), jnp.float32),
            pltpu.VMEM((3, heads * rows, TILE), jnp.float32),
            pltpu.VMEM((2, rows, q_half), jnp.bfloat16),
            pltpu.VMEM((n, 1, TILE), jnp.int32),
            pltpu.SMEM(tile_order.shape, jnp.int32),
            pltpu.SMEM(exit_layer.shape, jnp.int32),
            pltpu.SMEM((1,), jnp.int32),
            dma((2,)),
            dma((2,)),
            dma((3,)),
            dma((2, 2)),
            dma((n, 2, tiles)),
            dma((2,)),
            dma((3,)),
            dma((n,)),
            pltpu.SemaphoreType.REGULAR,
        ],
        compiler_params=pltpu.CompilerParams(
            collective_id=0, has_side_effects=True, vmem_limit_bytes=62_500_000
        ),
        name="attend_line",
    )(
        tile_order, exit_layer, queries[0],
        keys.reshape(tiles, TILE, kv_width), values.reshape(tiles, TILE, kv_width),
    )
    return attended[None], live


def solution(mesh):
    return jax.shard_map(
        functools.partial(body, mesh.shape["seq"]),
        mesh=mesh,
        in_specs=(
            P(None, ("batch", "seq"), "head"),
            P(None, ("batch", "seq"), "head"),
            P(None, ("batch", "seq"), "head"),
            P(("batch", "seq")),
            P("batch"),
        ),
        out_specs=(P(None, ("batch", "seq"), "head"), P("batch")),
        check_vma=False,
    )
```

```python
import functools
import math

import jax
import jax.numpy as jnp
from jax import lax
from jax.experimental import pallas as pl
from jax.experimental.pallas import tpu as pltpu
from jax.sharding import PartitionSpec as P

HD = 256
TILE = 128
SOFTCAP = 50.0
QUERY_SCALE = 0.0625
IN_SCALE = QUERY_SCALE / SOFTCAP
OUT_SCALE = SOFTCAP * math.log2(math.e)
MESH = pl.DeviceIdType.MESH
SERVED, SPREAD = 0, 1
GATE_A, GATE_B, AHEAD = 2, 2, 1


def kernel(
    n, order_hbm, exit_hbm, q_hbm, k_hbm, v_hbm, out_ref, exits,
    qb, kv, acc, den, done, order_ref, exit_ref, kv_sem, q_sem,
    small_sem, send_sem, recv_sem, pair_send, pair_recv, exit_recv, ready,
):
    me = lax.axis_index("seq")
    core = lax.axis_index("head")
    tiles = kv.shape[2]
    heads, rows = qb.shape[1:3]
    q_half = heads * HD
    far = n - 1
    at_end = (me == 0) | (me == far)
    serves = (me == 1) | (me == far - 1)
    end = jnp.where(me < n // 2, 0, far)
    inward = jnp.where(me < n // 2, 1, -1)
    first = core

    def inside(owner):
        return (owner >= 0) & (owner < n)

    def peer(step):
        return {"seq": jnp.clip(me + step, 0, far)}

    def load_own(hh):
        for which, src in enumerate((k_hbm, v_hbm)):
            pltpu.make_async_copy(
                src.at[:, :, pl.ds(pl.multiple_of(hh * HD, HD), HD)],
                kv.at[me, hh, :, which],
                kv_sem.at[hh],
            ).start()

    def wait_own(hh):
        pltpu.make_async_copy(kv.at[me, hh], kv.at[me, hh], kv_sem.at[hh]).wait()

    def load_queries(hh):
        for h in range(heads):
            pltpu.make_async_copy(
                q_hbm.at[:, pl.ds(hh * q_half + h * HD, HD)], qb.at[hh, h], q_sem.at[hh]
            ).start()

    def wait_queries(hh):
        pltpu.make_async_copy(qb.at[hh], qb.at[hh], q_sem.at[hh]).wait()

    small = [
        pltpu.make_async_copy(exit_hbm, exit_ref, small_sem.at[0]),
        pltpu.make_async_copy(order_hbm, order_ref, small_sem.at[1]),
    ]

    barrier = pltpu.get_barrier_semaphore()

    @pl.when(inside(me + 1))
    def _():
        pl.semaphore_signal(barrier, inc=1, device_id=peer(1), device_id_type=MESH)

    small[0].start()
    load_own(first)
    asks = at_end & (core == 0)

    @pl.when(asks)
    def _():
        load_queries(0)

    small[0].wait()
    lane = lax.broadcasted_iota(jnp.int32, (1, TILE), 1)
    mine = jnp.zeros((1, TILE), jnp.int32)
    for i in range(tiles):
        mine = jnp.where(lane == i, exit_ref[i], mine)
    exits[me] = mine

    @pl.when(inside(me - 1))
    def _():
        pl.semaphore_wait(barrier, 1)
        pl.semaphore_signal(ready, inc=1, device_id=peer(-1), device_id_type=MESH)

    soon = min(AHEAD, tiles - 1)

    def hop(owner, hh, t, step):
        return pltpu.make_async_remote_copy(
            src_ref=kv.at[owner, hh, t],
            dst_ref=kv.at[owner, hh, t],
            send_sem=send_sem.at[0, jnp.where(step > 0, 1, 0)],
            recv_sem=recv_sem.at[owner, hh, t],
            device_id=peer(step),
            device_id_type=MESH,
        )

    def exit_hop(owner, step):
        return pltpu.make_async_remote_copy(
            src_ref=exits.at[owner],
            dst_ref=exits.at[owner],
            send_sem=send_sem.at[1, jnp.where(step > 0, 1, 0)],
            recv_sem=exit_recv.at[owner],
            device_id=peer(step),
            device_id_type=MESH,
        )

    def goes(hh, step):
        room = jnp.where(step > 0, far - me, me)
        return (room > 1) | ((room == 1) & (hh == SPREAD))

    def send(owner, hh, t, step):
        @pl.when(goes(hh, step))
        def _():
            hop(owner, hh, t, step).start()

    def send_own(hh, step, low=0, high=tiles):
        @pl.loop(low, high)
        def _(t):
            send(me, hh, t, step)

    def query_copy():
        return pltpu.make_async_remote_copy(
            src_ref=qb.at[0], dst_ref=qb.at[2],
            send_sem=pair_send.at[0], recv_sem=pair_recv.at[0],
            device_id=peer(inward), device_id_type=MESH,
        )

    def done_copy(low, count, last):
        part = pl.ds(low * TILE, count * TILE)
        return pltpu.make_async_remote_copy(
            src_ref=done.at[0, part], dst_ref=done.at[1, part],
            send_sem=pair_send.at[1], recv_sem=pair_recv.at[2 if last else 1],
            device_id=peer(-inward), device_id_type=MESH,
        )

    def open_side(step):
        exit_hop(me, step).start()

        @pl.when(~at_end)
        def _():
            send_own(first, step)

        @pl.when(at_end & (core == 0))
        def _():
            query_copy().start()
            send_own(SERVED, step)

        @pl.when(at_end & (core == 1))
        def _():
            send_own(SPREAD, step, 0, soon)

    @pl.when(asks)
    def _():
        wait_queries(0)

    wait_own(first)

    @pl.when(inside(me - 1))
    def _():
        open_side(-1)

    @pl.when(inside(me + 1))
    def _():
        pl.semaphore_wait(ready, 1)
        open_side(1)

    load_own(1 - first)
    load_queries(1)
    small[1].start()

    @pl.when(~asks)
    def _():
        load_queries(0)

    wait_own(1 - first)

    @pl.when(~at_end)
    def _():
        send_own(1 - first, -inward)

    acc[...] = jnp.zeros_like(acc)
    den[...] = jnp.zeros_like(den)

    @pl.when(~asks)
    def _():
        wait_queries(0)

    wait_queries(1)
    small[1].wait()
    ahead = lax.broadcasted_iota(jnp.int32, (TILE, TILE), 1) - lax.broadcasted_iota(
        jnp.int32, (TILE, TILE), 0
    )

    def fold_into(slot, row_owner, owner, hh, t):
        key_place = order_ref[owner * tiles + t]
        over = jnp.stack(
            [
                ahead - (order_ref[row_owner * tiles + i] - key_place) * TILE
                for i in range(tiles)
            ]
        )
        stacked = (heads * rows, HD)
        scores = lax.dot_general(
            qb[slot].reshape(stacked), kv[owner, hh, t, 0],
            (((1,), (1,)), ((), ())), preferred_element_type=jnp.float32,
        ).reshape(heads, tiles, TILE, TILE)
        weights = jnp.where(
            over[None] <= 0, jnp.exp2(OUT_SCALE * jnp.tanh(scores * IN_SCALE)), 0.0
        ).reshape(heads * rows, TILE)
        den[slot] += weights
        acc[slot] += jnp.dot(
            weights.astype(jnp.bfloat16), kv[owner, hh, t, 1],
            preferred_element_type=jnp.float32,
        )

    def finish(slot, i, h):
        here = pl.ds(h * rows + i * TILE, TILE)
        total = jnp.sum(den[slot, here, :], axis=1, keepdims=True)
        return (acc[slot, here, :] / total).astype(jnp.bfloat16)

    def live_only(i, rows_out):
        return jnp.where(exit_ref[i] > 0, rows_out, jnp.zeros_like(rows_out))

    def keep(slot, i, h):
        out_ref[pl.ds(i * TILE, TILE), pl.ds(slot * q_half + h * HD, HD)] = live_only(
            i, finish(slot, i, h)
        )

    @pl.loop(jnp.where(at_end, tiles * (1 - core), 0), jnp.where(at_end, tiles * (2 - core), 2 * tiles))
    def _(k):
        hh = jnp.where(k < tiles, first, 1 - first)
        fold_into(hh, me, me, hh, lax.rem(k, tiles))

    def arrive(owner, hh, t, side):
        hop(owner, hh, t, side).wait_recv()
        send(owner, hh, t, -side)

        @pl.when((hh == SPREAD) & (t == 0))
        def _():
            exit_hop(owner, side).wait_recv()

            @pl.when(inside(me - side))
            def _():
                exit_hop(owner, -side).start()

    def collect(i):
        here = pl.ds(i * TILE, TILE)
        out_ref[here, pl.ds(0, q_half)] = live_only(i, done[1, here, :])

    def finish_served():
        for t in range(tiles):
            for h in range(heads):
                done[0, pl.ds(t * TILE, TILE), pl.ds(h * HD, HD)] = finish(2, t, h)
            if t > 0:
                done_copy(t - 1, 1, False).start()

        @pl.when(core == 0)
        def _():
            for h in range(heads):
                keep(0, 0, h)
            done_copy(tiles - 1, 1, True).start()

    early = core == 0

    @pl.loop(0, 3 * far - 1)
    def _(u):
        spread_a = u >= far
        s_a = jnp.where(spread_a, u - far + 1, u + 1)
        served_b = (u >= far) & (u < 2 * far)
        late_b = u >= 2 * far
        s_b = jnp.where(late_b, u - 2 * far + 2, jnp.where(served_b, u - far + 1, u + 1))
        hh_in = jnp.where(early, spread_a, ~served_b).astype(jnp.int32)
        s_in = jnp.where(early, s_a, s_b)
        extra = serves & (u == far + 1)
        hh_out = jnp.where(early, spread_a, ~served_b | extra).astype(jnp.int32)
        s_out = jnp.where(early, s_a, jnp.where(extra, 1, jnp.where(late_b, s_b - 1, s_b)))
        part_in = ~early & (u > 0) & (hh_in == SPREAD)
        low_in = jnp.where(part_in & late_b, soon, 0)
        high_in = jnp.where(part_in & ~late_b, soon, tiles)
        part_out = ~early & (hh_out == SPREAD)
        low_out = jnp.where(part_out & (late_b | extra), soon, 0)
        high_out = jnp.where(part_out & ~(late_b | extra), soon, tiles)
        from_in = me + inward * s_in
        from_out = me - inward * s_out
        runs = ~early | (u < 2 * far)
        any_in = runs & inside(from_in) & ~(at_end & (hh_in == SERVED))
        any_out = runs & inside(from_out) & ~at_end & ~(late_b & ~early & serves)
        later = early & ~at_end & (hh_in == SERVED)
        both = early & ~at_end & (hh_in == SPREAD)
        serving = runs & serves & (hh_in == SERVED) & inside(from_in)

        @pl.when(any_in | any_out)
        def _():
            @pl.loop(0, tiles)
            def _(t):
                has_in = any_in & (t >= low_in) & (t < high_in)
                has_out = any_out & (t >= low_out) & (t < high_out)

                @pl.when((u == jnp.where(early, 2 * far - 1, 3 * far - 2)) & (t == tiles - 1) & at_end)
                def _():
                    done_copy(0, tiles - 1, False).wait_recv()
                    for i in range(tiles - 1):
                        collect(i)

                @pl.when(has_out)
                def _():
                    arrive(from_out, hh_out, t, -inward)

                @pl.when(has_in)
                def _():
                    arrive(from_in, hh_in, t, inward)

                @pl.when(~early & serves & (u == 2 * far) & (t == tiles - 1))
                def _():
                    done_copy(tiles - 1, 1, True).start()

                @pl.when(early & ~at_end & (u == 0) & (t == tiles - 1))
                def _():
                    send_own(SPREAD, inward)

                @pl.when(~early & ~at_end & (u == 0) & (t == soon - 1))
                def _():
                    send_own(SERVED, inward)

                @pl.when(~early & at_end & (u == 0) & (t == GATE_B))
                def _():
                    query_copy().start()
                    send_own(SERVED, inward)
                    send_own(SPREAD, inward, soon, tiles)

                @pl.when(early & at_end & (u == far) & (t == GATE_A))
                def _():
                    send_own(SPREAD, inward)

                @pl.when(serving & (s_in == 1) & (t == 0))
                def _():
                    query_copy().wait_recv()

                @pl.loop(0, jnp.where(serving, jnp.where(s_in == 1, 3, 1), 0))
                def _(k):
                    owner = jnp.where(k == 2, me, jnp.where(k == 1, from_out, from_in))
                    fold_into(2, end, owner, SERVED, t)

                @pl.when(serving & (s_in == far - 1) & (t == tiles - 1))
                def _():
                    finish_served()

                @pl.loop(jnp.where(has_in, 0, 1), jnp.where(both, 4, 2))
                def _(k):
                    outer = (k % 2) == 1

                    @pl.when(jnp.where(outer, has_out, has_in) & ~later)
                    def _():
                        hh = jnp.where(k > 1, SERVED, jnp.where(outer, hh_out, hh_in))
                        fold_into(hh, me, jnp.where(outer, from_out, from_in), hh, t)

    for i in range(tiles):
        for h in range(heads):
            keep(1, i, h)

    @pl.when(~at_end)
    def _():
        for i in range(tiles):
            for h in range(heads):
                keep(0, i, h)

    @pl.when(at_end)
    def _():
        done_copy(tiles - 1, 1, True).wait_recv()
        collect(tiles - 1)
        query_copy().wait_send()

    @pl.when(serves)
    def _():
        done_copy(0, tiles, True).wait_send()

    for step in (1, -1):
        room = jnp.where(step > 0, far - me, me)
        count = n - room

        def sent(ref, row):
            return pltpu.make_async_remote_copy(
                src_ref=ref, dst_ref=ref,
                send_sem=send_sem.at[row, (step + 1) // 2], recv_sem=exit_recv.at[0],
                device_id=peer(step), device_id_type=MESH,
            )

        @pl.when(room == 1)
        def _():
            sent(kv.at[pl.ds(0, far), SPREAD], 0).wait_send()

        for c in range(1, n):
            @pl.when(count == c)
            def _():
                sent(exits.at[pl.ds(0, c)], 1).wait_send()

            if c < far:
                @pl.when(count == c)
                def _():
                    sent(kv.at[pl.ds(0, c)], 0).wait_send()


def write_out(attended, exits, out_hbm, live_hbm, live, sems):
    whole = pltpu.make_async_copy(attended, out_hbm.at[0], sems.at[0])
    whole.start()
    live[0] = jnp.sum((exits[...] > 0).astype(jnp.int32))
    count = pltpu.make_async_copy(live, live_hbm, sems.at[1])
    count.start()
    count.wait()
    whole.wait()


def body(n, queries, keys, values, exit_layer, tile_order):
    rows, q_width = queries.shape[1:]
    kv_width = keys.shape[2]
    q_half = q_width // 2
    heads = q_half // HD
    tiles = rows // TILE
    hbm = pl.BlockSpec(memory_space=pltpu.HBM)
    vmem = pl.BlockSpec(memory_space=pltpu.VMEM)
    dma = pltpu.SemaphoreType.DMA
    attended, exits = pl.pallas_call(
        functools.partial(kernel, n),
        out_shape=(
            pltpu.VMEM((rows, q_width), jnp.bfloat16),
            pltpu.VMEM((n, 1, TILE), jnp.int32),
        ),
        in_specs=[hbm] * 5,
        out_specs=(vmem, vmem),
        scratch_shapes=[
            pltpu.VMEM((3, heads, rows, HD), jnp.bfloat16),
            pltpu.VMEM((n, 2, tiles, 2, TILE, HD), jnp.bfloat16),
            pltpu.VMEM((3, heads * rows, HD), jnp.float32),
            pltpu.VMEM((3, heads * rows, TILE), jnp.float32),
            pltpu.VMEM((2, rows, q_half), jnp.bfloat16),
            pltpu.SMEM(tile_order.shape, jnp.int32),
            pltpu.SMEM(exit_layer.shape, jnp.int32),
            dma((2,)),
            dma((2,)),
            dma((2,)),
            dma((2, 2)),
            dma((n, 2, tiles)),
            dma((2,)),
            dma((3,)),
            dma((n,)),
            pltpu.SemaphoreType.REGULAR,
        ],
        compiler_params=pltpu.CompilerParams(
            collective_id=0, has_side_effects=True, vmem_limit_bytes=62_000_000
        ),
        name="attend_line",
    )(
        tile_order, exit_layer, queries[0],
        keys.reshape(tiles, TILE, kv_width), values.reshape(tiles, TILE, kv_width),
    )
    return pl.pallas_call(
        write_out,
        out_shape=(
            jax.ShapeDtypeStruct((1, rows, q_width), jnp.bfloat16),
            jax.ShapeDtypeStruct((1,), jnp.int32),
        ),
        in_specs=[vmem, vmem],
        out_specs=(hbm, hbm),
        scratch_shapes=[pltpu.SMEM((1,), jnp.int32), dma((2,))],
        compiler_params=pltpu.CompilerParams(vmem_limit_bytes=1_000_000),
        name="write_out",
    )(attended, exits)


def solution(mesh):
    return jax.shard_map(
        functools.partial(body, mesh.shape["seq"]),
        mesh=mesh,
        in_specs=(
            P(None, ("batch", "seq"), "head"),
            P(None, ("batch", "seq"), "head"),
            P(None, ("batch", "seq"), "head"),
            P(("batch", "seq")),
            P("batch"),
        ),
        out_specs=(P(None, ("batch", "seq"), "head"), P("batch")),
        check_vma=False,
    )
```

```python
import functools
import math

import jax
import jax.numpy as jnp
from jax import lax
from jax.experimental import pallas as pl
from jax.experimental.pallas import tpu as pltpu
from jax.sharding import PartitionSpec as P

HD = 256
TILE = 128
SOFTCAP = 50.0
QUERY_SCALE = 0.0625
IN_SCALE = QUERY_SCALE / SOFTCAP
OUT_SCALE = SOFTCAP * math.log2(math.e)
MESH = pl.DeviceIdType.MESH
SERVED, SPREAD = 0, 1
GATE_A, GATE_B, AHEAD = 2, 2, 1


def kernel(
    n, order_hbm, exit_hbm, q_hbm, k_hbm, v_hbm, out_ref, exits,
    qb, kv, acc, den, done, order_ref, exit_ref, kv_sem, q_sem,
    small_sem, send_sem, recv_sem, pair_send, pair_recv, exit_recv, ready,
):
    me = lax.axis_index("seq")
    core = lax.axis_index("head")
    tiles = kv.shape[2]
    heads, rows = qb.shape[1:3]
    q_half = heads * HD
    far = n - 1
    at_end = (me == 0) | (me == far)
    serves = (me == 1) | (me == far - 1)
    end = jnp.where(me < n // 2, 0, far)
    inward = jnp.where(me < n // 2, 1, -1)
    first = core

    def inside(owner):
        return (owner >= 0) & (owner < n)

    def peer(step):
        return {"seq": jnp.clip(me + step, 0, far)}

    def load_own(hh, low, high, sem):
        here = pl.ds(low, high - low)
        for which, src in enumerate((k_hbm, v_hbm)):
            pltpu.make_async_copy(
                src.at[here, :, pl.ds(pl.multiple_of(hh * HD, HD), HD)],
                kv.at[me, hh, here, which],
                kv_sem.at[sem],
            ).start()

    def wait_own(hh, low, high, sem):
        part = kv.at[me, hh, pl.ds(low, high - low)]
        pltpu.make_async_copy(part, part, kv_sem.at[sem]).wait()

    def load_queries(hh):
        for h in range(heads):
            pltpu.make_async_copy(
                q_hbm.at[:, pl.ds(hh * q_half + h * HD, HD)], qb.at[hh, h], q_sem.at[hh]
            ).start()

    def wait_queries(hh):
        pltpu.make_async_copy(qb.at[hh], qb.at[hh], q_sem.at[hh]).wait()

    small = [
        pltpu.make_async_copy(exit_hbm, exit_ref, small_sem.at[0]),
        pltpu.make_async_copy(order_hbm, order_ref, small_sem.at[1]),
    ]

    barrier = pltpu.get_barrier_semaphore()

    @pl.when(inside(me + 1))
    def _():
        pl.semaphore_signal(barrier, inc=1, device_id=peer(1), device_id_type=MESH)

    load_own(first, 0, 1, 2)
    small[0].start()
    asks = at_end & (core == 0)

    @pl.when(asks)
    def _():
        load_queries(0)

    load_own(first, 1, tiles, first)
    @pl.when(inside(me - 1))
    def _():
        pl.semaphore_wait(barrier, 1)
        pl.semaphore_signal(ready, inc=1, device_id=peer(-1), device_id_type=MESH)

    soon = min(AHEAD, tiles - 1)

    def hop(owner, hh, t, step):
        return pltpu.make_async_remote_copy(
            src_ref=kv.at[owner, hh, t],
            dst_ref=kv.at[owner, hh, t],
            send_sem=send_sem.at[0, jnp.where(step > 0, 1, 0)],
            recv_sem=recv_sem.at[owner, hh, t],
            device_id=peer(step),
            device_id_type=MESH,
        )

    def exit_hop(owner, step):
        return pltpu.make_async_remote_copy(
            src_ref=exits.at[owner],
            dst_ref=exits.at[owner],
            send_sem=send_sem.at[1, jnp.where(step > 0, 1, 0)],
            recv_sem=exit_recv.at[owner],
            device_id=peer(step),
            device_id_type=MESH,
        )

    def goes(hh, step):
        room = jnp.where(step > 0, far - me, me)
        return (room > 1) | ((room == 1) & (hh == SPREAD))

    def send(owner, hh, t, step):
        @pl.when(goes(hh, step))
        def _():
            hop(owner, hh, t, step).start()

    def send_own(hh, step, low=0, high=tiles):
        @pl.loop(low, high)
        def _(t):
            send(me, hh, t, step)

    def query_copy():
        return pltpu.make_async_remote_copy(
            src_ref=qb.at[0], dst_ref=qb.at[2],
            send_sem=pair_send.at[0], recv_sem=pair_recv.at[0],
            device_id=peer(inward), device_id_type=MESH,
        )

    def done_copy(low, count, last):
        part = pl.ds(low * TILE, count * TILE)
        return pltpu.make_async_remote_copy(
            src_ref=done.at[0, part], dst_ref=done.at[1, part],
            send_sem=pair_send.at[1], recv_sem=pair_recv.at[2 if last else 1],
            device_id=peer(-inward), device_id_type=MESH,
        )

    def push(step, low, high):
        @pl.when(~at_end)
        def _():
            send_own(first, step, low, high)

        @pl.when(asks)
        def _():
            if low == 0:
                query_copy().start()
            send_own(SERVED, step, low, high)

    @pl.when(asks)
    def _():
        wait_queries(0)

    wait_own(first, 0, 1, 2)

    @pl.when(inside(me - 1))
    def _():
        push(-1, 0, 1)

    small[0].wait()
    lane = lax.broadcasted_iota(jnp.int32, (1, TILE), 1)
    mine = jnp.zeros((1, TILE), jnp.int32)
    for i in range(tiles):
        mine = jnp.where(lane == i, exit_ref[i], mine)
    exits[me] = mine

    @pl.when(inside(me - 1))
    def _():
        exit_hop(me, -1).start()

    wait_own(first, 1, tiles, first)

    @pl.when(inside(me - 1))
    def _():
        push(-1, 1, tiles)

    @pl.when(inside(me + 1))
    def _():
        pl.semaphore_wait(ready, 1)
        exit_hop(me, 1).start()
        push(1, 0, tiles)

    @pl.when(at_end & (core == 1))
    def _():
        send_own(SPREAD, inward, 0, soon)

    load_own(1 - first, 0, tiles, 1 - first)
    load_queries(1)
    small[1].start()

    @pl.when(~asks)
    def _():
        load_queries(0)

    wait_own(1 - first, 0, tiles, 1 - first)

    @pl.when(~at_end)
    def _():
        send_own(1 - first, -inward)

    acc[...] = jnp.zeros_like(acc)
    den[...] = jnp.zeros_like(den)

    @pl.when(~asks)
    def _():
        wait_queries(0)

    wait_queries(1)
    small[1].wait()
    ahead = lax.broadcasted_iota(jnp.int32, (TILE, TILE), 1) - lax.broadcasted_iota(
        jnp.int32, (TILE, TILE), 0
    )

    def fold_into(slot, row_owner, owner, hh, t):
        key_place = order_ref[owner * tiles + t]
        over = jnp.stack(
            [
                ahead - (order_ref[row_owner * tiles + i] - key_place) * TILE
                for i in range(tiles)
            ]
        )
        stacked = (heads * rows, HD)
        scores = lax.dot_general(
            qb[slot].reshape(stacked), kv[owner, hh, t, 0],
            (((1,), (1,)), ((), ())), preferred_element_type=jnp.float32,
        ).reshape(heads, tiles, TILE, TILE)
        weights = jnp.where(
            over[None] <= 0, jnp.exp2(OUT_SCALE * jnp.tanh(scores * IN_SCALE)), 0.0
        ).reshape(heads * rows, TILE)
        den[slot] += weights
        acc[slot] += jnp.dot(
            weights.astype(jnp.bfloat16), kv[owner, hh, t, 1],
            preferred_element_type=jnp.float32,
        )

    def finish(slot, i, h):
        here = pl.ds(h * rows + i * TILE, TILE)
        total = jnp.sum(den[slot, here, :], axis=1, keepdims=True)
        return (acc[slot, here, :] / total).astype(jnp.bfloat16)

    def live_only(i, rows_out):
        return jnp.where(exit_ref[i] > 0, rows_out, jnp.zeros_like(rows_out))

    def keep(slot, i, h):
        out_ref[pl.ds(i * TILE, TILE), pl.ds(slot * q_half + h * HD, HD)] = live_only(
            i, finish(slot, i, h)
        )

    @pl.loop(jnp.where(at_end, tiles * (1 - core), 0), jnp.where(at_end, tiles * (2 - core), 2 * tiles))
    def _(k):
        hh = jnp.where(k < tiles, first, 1 - first)
        fold_into(hh, me, me, hh, lax.rem(k, tiles))

    def arrive(owner, hh, t, side):
        hop(owner, hh, t, side).wait_recv()
        send(owner, hh, t, -side)

        @pl.when((hh == SPREAD) & (t == 0))
        def _():
            exit_hop(owner, side).wait_recv()

            @pl.when(inside(me - side))
            def _():
                exit_hop(owner, -side).start()

    def collect(i):
        here = pl.ds(i * TILE, TILE)
        out_ref[here, pl.ds(0, q_half)] = live_only(i, done[1, here, :])

    def finish_served():
        for t in range(tiles):
            for h in range(heads):
                done[0, pl.ds(t * TILE, TILE), pl.ds(h * HD, HD)] = finish(2, t, h)
            if t > 0:
                done_copy(t - 1, 1, False).start()

        @pl.when(core == 0)
        def _():
            for h in range(heads):
                keep(0, 0, h)
            done_copy(tiles - 1, 1, True).start()

    early = core == 0

    @pl.loop(0, 3 * far - 1)
    def _(u):
        spread_a = u >= far
        s_a = jnp.where(spread_a, u - far + 1, u + 1)
        served_b = (u >= far) & (u < 2 * far)
        late_b = u >= 2 * far
        s_b = jnp.where(late_b, u - 2 * far + 2, jnp.where(served_b, u - far + 1, u + 1))
        hh_in = jnp.where(early, spread_a, ~served_b).astype(jnp.int32)
        s_in = jnp.where(early, s_a, s_b)
        extra = serves & (u == far + 1)
        hh_out = jnp.where(early, spread_a, ~served_b | extra).astype(jnp.int32)
        s_out = jnp.where(early, s_a, jnp.where(extra, 1, jnp.where(late_b, s_b - 1, s_b)))
        part_in = ~early & (u > 0) & (hh_in == SPREAD)
        low_in = jnp.where(part_in & late_b, soon, 0)
        high_in = jnp.where(part_in & ~late_b, soon, tiles)
        part_out = ~early & (hh_out == SPREAD)
        low_out = jnp.where(part_out & (late_b | extra), soon, 0)
        high_out = jnp.where(part_out & ~(late_b | extra), soon, tiles)
        from_in = me + inward * s_in
        from_out = me - inward * s_out
        runs = ~early | (u < 2 * far)
        any_in = runs & inside(from_in) & ~(at_end & (hh_in == SERVED))
        any_out = runs & inside(from_out) & ~at_end & ~(late_b & ~early & serves)
        later = early & ~at_end & (hh_in == SERVED)
        both = early & ~at_end & (hh_in == SPREAD)
        serving = runs & serves & (hh_in == SERVED) & inside(from_in)

        @pl.when(any_in | any_out)
        def _():
            @pl.loop(0, tiles)
            def _(t):
                has_in = any_in & (t >= low_in) & (t < high_in)
                has_out = any_out & (t >= low_out) & (t < high_out)

                @pl.when((u == jnp.where(early, 2 * far - 1, 3 * far - 2)) & (t == tiles - 1) & at_end)
                def _():
                    done_copy(0, tiles - 1, False).wait_recv()
                    for i in range(tiles - 1):
                        collect(i)

                @pl.when(has_out)
                def _():
                    arrive(from_out, hh_out, t, -inward)

                @pl.when(has_in)
                def _():
                    arrive(from_in, hh_in, t, inward)

                @pl.when(~early & serves & (u == 2 * far) & (t == tiles - 1))
                def _():
                    done_copy(tiles - 1, 1, True).start()

                @pl.when(early & ~at_end & (u == 0) & (t == tiles - 1))
                def _():
                    send_own(SPREAD, inward)

                @pl.when(~early & ~at_end & (u == 0) & (t == soon - 1))
                def _():
                    send_own(SERVED, inward)

                @pl.when(~early & at_end & (u == 0) & (t == GATE_B))
                def _():
                    query_copy().start()
                    send_own(SERVED, inward)
                    send_own(SPREAD, inward, soon, tiles)

                @pl.when(early & at_end & (u == far) & (t == GATE_A))
                def _():
                    send_own(SPREAD, inward)

                @pl.when(serving & (s_in == 1) & (t == 0))
                def _():
                    query_copy().wait_recv()

                @pl.loop(0, jnp.where(serving, jnp.where(s_in == 1, 3, 1), 0))
                def _(k):
                    owner = jnp.where(k == 2, me, jnp.where(k == 1, from_out, from_in))
                    fold_into(2, end, owner, SERVED, t)

                @pl.when(serving & (s_in == far - 1) & (t == tiles - 1))
                def _():
                    finish_served()

                @pl.loop(jnp.where(has_in, 0, 1), jnp.where(both, 4, 2))
                def _(k):
                    outer = (k % 2) == 1

                    @pl.when(jnp.where(outer, has_out, has_in) & ~later)
                    def _():
                        hh = jnp.where(k > 1, SERVED, jnp.where(outer, hh_out, hh_in))
                        fold_into(hh, me, jnp.where(outer, from_out, from_in), hh, t)

    for i in range(tiles):
        for h in range(heads):
            keep(1, i, h)

    @pl.when(~at_end)
    def _():
        for i in range(tiles):
            for h in range(heads):
                keep(0, i, h)

    @pl.when(at_end)
    def _():
        done_copy(tiles - 1, 1, True).wait_recv()
        collect(tiles - 1)
        query_copy().wait_send()

    @pl.when(serves)
    def _():
        done_copy(0, tiles, True).wait_send()

    for step in (1, -1):
        room = jnp.where(step > 0, far - me, me)
        count = n - room

        def sent(ref, row):
            return pltpu.make_async_remote_copy(
                src_ref=ref, dst_ref=ref,
                send_sem=send_sem.at[row, (step + 1) // 2], recv_sem=exit_recv.at[0],
                device_id=peer(step), device_id_type=MESH,
            )

        @pl.when(room == 1)
        def _():
            sent(kv.at[pl.ds(0, far), SPREAD], 0).wait_send()

        for c in range(1, n):
            @pl.when(count == c)
            def _():
                sent(exits.at[pl.ds(0, c)], 1).wait_send()

            if c < far:
                @pl.when(count == c)
                def _():
                    sent(kv.at[pl.ds(0, c)], 0).wait_send()


def write_out(attended, exits, out_hbm, live_hbm, live, sems):
    whole = pltpu.make_async_copy(attended, out_hbm.at[0], sems.at[0])
    whole.start()
    live[0] = jnp.sum((exits[...] > 0).astype(jnp.int32))
    count = pltpu.make_async_copy(live, live_hbm, sems.at[1])
    count.start()
    count.wait()
    whole.wait()


def body(n, queries, keys, values, exit_layer, tile_order):
    rows, q_width = queries.shape[1:]
    kv_width = keys.shape[2]
    q_half = q_width // 2
    heads = q_half // HD
    tiles = rows // TILE
    hbm = pl.BlockSpec(memory_space=pltpu.HBM)
    vmem = pl.BlockSpec(memory_space=pltpu.VMEM)
    dma = pltpu.SemaphoreType.DMA
    attended, exits = pl.pallas_call(
        functools.partial(kernel, n),
        out_shape=(
            pltpu.VMEM((rows, q_width), jnp.bfloat16),
            pltpu.VMEM((n, 1, TILE), jnp.int32),
        ),
        in_specs=[hbm] * 5,
        out_specs=(vmem, vmem),
        scratch_shapes=[
            pltpu.VMEM((3, heads, rows, HD), jnp.bfloat16),
            pltpu.VMEM((n, 2, tiles, 2, TILE, HD), jnp.bfloat16),
            pltpu.VMEM((3, heads * rows, HD), jnp.float32),
            pltpu.VMEM((3, heads * rows, TILE), jnp.float32),
            pltpu.VMEM((2, rows, q_half), jnp.bfloat16),
            pltpu.SMEM(tile_order.shape, jnp.int32),
            pltpu.SMEM(exit_layer.shape, jnp.int32),
            dma((3,)),
            dma((2,)),
            dma((2,)),
            dma((2, 2)),
            dma((n, 2, tiles)),
            dma((2,)),
            dma((3,)),
            dma((n,)),
            pltpu.SemaphoreType.REGULAR,
        ],
        compiler_params=pltpu.CompilerParams(
            collective_id=0, has_side_effects=True, vmem_limit_bytes=62_000_000
        ),
        name="attend_line",
    )(
        tile_order, exit_layer, queries[0],
        keys.reshape(tiles, TILE, kv_width), values.reshape(tiles, TILE, kv_width),
    )
    return pl.pallas_call(
        write_out,
        out_shape=(
            jax.ShapeDtypeStruct((1, rows, q_width), jnp.bfloat16),
            jax.ShapeDtypeStruct((1,), jnp.int32),
        ),
        in_specs=[vmem, vmem],
        out_specs=(hbm, hbm),
        scratch_shapes=[pltpu.SMEM((1,), jnp.int32), dma((2,))],
        compiler_params=pltpu.CompilerParams(vmem_limit_bytes=1_000_000),
        name="write_out",
    )(attended, exits)


def solution(mesh):
    return jax.shard_map(
        functools.partial(body, mesh.shape["seq"]),
        mesh=mesh,
        in_specs=(
            P(None, ("batch", "seq"), "head"),
            P(None, ("batch", "seq"), "head"),
            P(None, ("batch", "seq"), "head"),
            P(("batch", "seq")),
            P("batch"),
        ),
        out_specs=(P(None, ("batch", "seq"), "head"), P("batch")),
        check_vma=False,
    )
```

```python
import functools
import math

import jax
import jax.numpy as jnp
from jax import lax
from jax.experimental import pallas as pl
from jax.experimental.pallas import tpu as pltpu
from jax.sharding import PartitionSpec as P

HD = 256
TILE = 128
SOFTCAP = 50.0
QUERY_SCALE = 0.0625
IN_SCALE = QUERY_SCALE / SOFTCAP
OUT_SCALE = SOFTCAP * math.log2(math.e)
MESH = pl.DeviceIdType.MESH
SERVED, SPREAD = 0, 1
AHEAD = 1


def kernel(
    n, order_hbm, exit_hbm, q_hbm, k_hbm, v_hbm, out_ref, exits,
    qb, kv, acc, den, done, order_ref, exit_ref, kv_sem, q_sem,
    small_sem, send_sem, recv_sem, pair_send, pair_recv, exit_recv, ready,
):
    me = lax.axis_index("seq")
    core = lax.axis_index("head")
    tiles = kv.shape[2]
    heads, rows = qb.shape[1:3]
    q_half = heads * HD
    far = n - 1
    at_end = (me == 0) | (me == far)
    serves = (me == 1) | (me == far - 1)
    end = jnp.where(me < n // 2, 0, far)
    inward = jnp.where(me < n // 2, 1, -1)
    first = core

    def inside(owner):
        return (owner >= 0) & (owner < n)

    def peer(step):
        return {"seq": jnp.clip(me + step, 0, far)}

    def load_own(hh, low, high, sem):
        here = pl.ds(low, high - low)
        for which, src in enumerate((k_hbm, v_hbm)):
            pltpu.make_async_copy(
                src.at[here, :, pl.ds(pl.multiple_of(hh * HD, HD), HD)],
                kv.at[me, hh, here, which],
                kv_sem.at[sem],
            ).start()

    def wait_own(hh, low, high, sem):
        part = kv.at[me, hh, pl.ds(low, high - low)]
        pltpu.make_async_copy(part, part, kv_sem.at[sem]).wait()

    def load_queries(hh):
        for h in range(heads):
            pltpu.make_async_copy(
                q_hbm.at[:, pl.ds(hh * q_half + h * HD, HD)], qb.at[hh, h], q_sem.at[hh]
            ).start()

    def wait_queries(hh):
        pltpu.make_async_copy(qb.at[hh], qb.at[hh], q_sem.at[hh]).wait()

    small = [
        pltpu.make_async_copy(exit_hbm, exit_ref, small_sem.at[0]),
        pltpu.make_async_copy(order_hbm, order_ref, small_sem.at[1]),
    ]

    barrier = pltpu.get_barrier_semaphore()

    @pl.when(inside(me + 1))
    def _():
        pl.semaphore_signal(barrier, inc=1, device_id=peer(1), device_id_type=MESH)

    load_own(first, 0, 1, 2)
    small[0].start()
    asks = at_end & (core == 0)

    @pl.when(asks)
    def _():
        load_queries(0)

    load_own(first, 1, tiles, first)
    @pl.when(inside(me - 1))
    def _():
        pl.semaphore_wait(barrier, 1)
        pl.semaphore_signal(ready, inc=1, device_id=peer(-1), device_id_type=MESH)

    soon = min(AHEAD, tiles - 1)

    def hop(owner, hh, t, step):
        return pltpu.make_async_remote_copy(
            src_ref=kv.at[owner, hh, t],
            dst_ref=kv.at[owner, hh, t],
            send_sem=send_sem.at[0, jnp.where(step > 0, 1, 0)],
            recv_sem=recv_sem.at[owner, hh, t],
            device_id=peer(step),
            device_id_type=MESH,
        )

    def exit_hop(owner, step):
        return pltpu.make_async_remote_copy(
            src_ref=exits.at[owner],
            dst_ref=exits.at[owner],
            send_sem=send_sem.at[1, jnp.where(step > 0, 1, 0)],
            recv_sem=exit_recv.at[owner],
            device_id=peer(step),
            device_id_type=MESH,
        )

    def goes(hh, step):
        room = jnp.where(step > 0, far - me, me)
        return (room > 1) | ((room == 1) & (hh == SPREAD))

    def send(owner, hh, t, step):
        @pl.when(goes(hh, step))
        def _():
            hop(owner, hh, t, step).start()

    def send_own(hh, step, low=0, high=tiles):
        @pl.loop(low, high)
        def _(t):
            send(me, hh, t, step)

    def query_copy():
        return pltpu.make_async_remote_copy(
            src_ref=qb.at[0], dst_ref=qb.at[2],
            send_sem=pair_send.at[0], recv_sem=pair_recv.at[0],
            device_id=peer(inward), device_id_type=MESH,
        )

    def done_copy(low, count, last):
        part = pl.ds(low * TILE, count * TILE)
        return pltpu.make_async_remote_copy(
            src_ref=done.at[0, part], dst_ref=done.at[1, part],
            send_sem=pair_send.at[1], recv_sem=pair_recv.at[2 if last else 1],
            device_id=peer(-inward), device_id_type=MESH,
        )

    def push(step, low, high):
        @pl.when(~at_end)
        def _():
            send_own(first, step, low, high)

        @pl.when(asks)
        def _():
            if low == 0:
                query_copy().start()
            send_own(SERVED, step, low, high)

    @pl.when(asks)
    def _():
        wait_queries(0)

    wait_own(first, 0, 1, 2)

    @pl.when(inside(me - 1))
    def _():
        push(-1, 0, 1)

    small[0].wait()
    lane = lax.broadcasted_iota(jnp.int32, (1, TILE), 1)
    mine = jnp.zeros((1, TILE), jnp.int32)
    for i in range(tiles):
        mine = jnp.where(lane == i, exit_ref[i], mine)
    exits[me] = mine

    @pl.when(inside(me - 1))
    def _():
        exit_hop(me, -1).start()

    wait_own(first, 1, tiles, first)

    @pl.when(inside(me - 1))
    def _():
        push(-1, 1, tiles)

    @pl.when(inside(me + 1))
    def _():
        pl.semaphore_wait(ready, 1)
        exit_hop(me, 1).start()
        push(1, 0, tiles)

    @pl.when(at_end & (core == 1))
    def _():
        send_own(SPREAD, inward, 0, soon)

    load_own(1 - first, 0, tiles, 1 - first)
    load_queries(1)
    small[1].start()

    @pl.when(~asks)
    def _():
        load_queries(0)

    wait_own(1 - first, 0, tiles, 1 - first)

    @pl.when(~at_end)
    def _():
        send_own(1 - first, -inward)

    acc[...] = jnp.zeros_like(acc)
    den[...] = jnp.zeros_like(den)

    @pl.when(~asks)
    def _():
        wait_queries(0)

    wait_queries(1)
    small[1].wait()
    ahead = lax.broadcasted_iota(jnp.int32, (TILE, TILE), 1) - lax.broadcasted_iota(
        jnp.int32, (TILE, TILE), 0
    )

    def fold_into(slot, row_owner, owner, hh, t):
        key_place = order_ref[owner * tiles + t]
        over = jnp.stack(
            [
                ahead - (order_ref[row_owner * tiles + i] - key_place) * TILE
                for i in range(tiles)
            ]
        )
        stacked = (heads * rows, HD)
        scores = lax.dot_general(
            qb[slot].reshape(stacked), kv[owner, hh, t, 0],
            (((1,), (1,)), ((), ())), preferred_element_type=jnp.float32,
        ).reshape(heads, tiles, TILE, TILE)
        weights = jnp.where(
            over[None] <= 0, jnp.exp2(OUT_SCALE * jnp.tanh(scores * IN_SCALE)), 0.0
        ).reshape(heads * rows, TILE)
        den[slot] += weights
        acc[slot] += jnp.dot(
            weights.astype(jnp.bfloat16), kv[owner, hh, t, 1],
            preferred_element_type=jnp.float32,
        )

    def finish(slot, i, h):
        here = pl.ds(h * rows + i * TILE, TILE)
        total = jnp.sum(den[slot, here, :], axis=1, keepdims=True)
        return (acc[slot, here, :] / total).astype(jnp.bfloat16)

    def live_only(i, rows_out):
        return jnp.where(exit_ref[i] > 0, rows_out, jnp.zeros_like(rows_out))

    def keep(slot, i, h):
        out_ref[pl.ds(i * TILE, TILE), pl.ds(slot * q_half + h * HD, HD)] = live_only(
            i, finish(slot, i, h)
        )

    @pl.loop(jnp.where(at_end, tiles * (1 - core), 0), jnp.where(at_end, tiles * (2 - core), 2 * tiles))
    def _(k):
        hh = jnp.where(k < tiles, first, 1 - first)
        fold_into(hh, me, me, hh, lax.rem(k, tiles))

    def arrive(owner, hh, t, side):
        hop(owner, hh, t, side).wait_recv()
        send(owner, hh, t, -side)

        @pl.when((hh == SPREAD) & (t == 0))
        def _():
            exit_hop(owner, side).wait_recv()

            @pl.when(inside(me - side))
            def _():
                exit_hop(owner, -side).start()

    def collect(i):
        here = pl.ds(i * TILE, TILE)
        out_ref[here, pl.ds(0, q_half)] = live_only(i, done[1, here, :])

    def finish_served(owner, t):
        key_place = order_ref[owner * tiles + t]
        for i in range(tiles):
            place = order_ref[end * tiles + i]
            part = pl.ds(i * TILE, TILE)
            scores = lax.dot_general(
                qb[2, :, part, :].reshape(heads * TILE, HD), kv[owner, SERVED, t, 0],
                (((1,), (1,)), ((), ())), preferred_element_type=jnp.float32,
            ).reshape(heads, TILE, TILE)
            weights = jnp.where(
                (ahead - (place - key_place) * TILE)[None] <= 0,
                jnp.exp2(OUT_SCALE * jnp.tanh(scores * IN_SCALE)), 0.0,
            )
            added = jnp.dot(
                weights.astype(jnp.bfloat16).reshape(heads * TILE, TILE),
                kv[owner, SERVED, t, 1], preferred_element_type=jnp.float32,
            ).reshape(heads, TILE, HD)
            for h in range(heads):
                here = pl.ds(h * rows + i * TILE, TILE)
                total = jnp.sum(den[2, here, :] + weights[h], axis=1, keepdims=True)
                done[0, part, pl.ds(h * HD, HD)] = (
                    (acc[2, here, :] + added[h]) / total
                ).astype(jnp.bfloat16)
            if i > 0:
                done_copy(i - 1, 1, False).start()

        @pl.when(core == 0)
        def _():
            for h in range(heads):
                keep(0, 0, h)
            done_copy(tiles - 1, 1, True).start()

    early = core == 0

    @pl.loop(0, 3 * far - 1)
    def _(u):
        spread_a = u >= far
        s_a = jnp.where(spread_a, u - far + 1, u + 1)
        served_b = (u >= far) & (u < 2 * far)
        late_b = u >= 2 * far
        s_b = jnp.where(late_b, u - 2 * far + 2, jnp.where(served_b, u - far + 1, u + 1))
        hh_in = jnp.where(early, spread_a, ~served_b).astype(jnp.int32)
        s_in = jnp.where(early, s_a, s_b)
        extra = serves & (u == far + 1)
        hh_out = jnp.where(early, spread_a, ~served_b | extra).astype(jnp.int32)
        s_out = jnp.where(early, s_a, jnp.where(extra, 1, jnp.where(late_b, s_b - 1, s_b)))
        part_in = ~early & (u > 0) & (hh_in == SPREAD)
        low_in = jnp.where(part_in & late_b, soon, 0)
        high_in = jnp.where(part_in & ~late_b, soon, tiles)
        part_out = ~early & (hh_out == SPREAD)
        low_out = jnp.where(part_out & (late_b | extra), soon, 0)
        high_out = jnp.where(part_out & ~(late_b | extra), soon, tiles)
        from_in = me + inward * s_in
        from_out = me - inward * s_out
        runs = ~early | (u < 2 * far)
        any_in = runs & inside(from_in) & ~(at_end & (hh_in == SERVED))
        any_out = runs & inside(from_out) & ~at_end & ~(late_b & ~early & serves)
        later = early & ~at_end & (hh_in == SERVED)
        both = early & ~at_end & (hh_in == SPREAD)
        serving = runs & serves & (hh_in == SERVED) & inside(from_in)

        @pl.when(any_in | any_out)
        def _():
            @pl.loop(0, tiles)
            def _(t):
                has_in = any_in & (t >= low_in) & (t < high_in)
                has_out = any_out & (t >= low_out) & (t < high_out)

                @pl.when((u == jnp.where(early, 2 * far - 1, 3 * far - 2)) & (t == tiles - 1) & at_end)
                def _():
                    done_copy(0, tiles - 1, False).wait_recv()
                    for i in range(tiles - 1):
                        collect(i)

                @pl.when(has_out)
                def _():
                    arrive(from_out, hh_out, t, -inward)

                @pl.when(has_in)
                def _():
                    arrive(from_in, hh_in, t, inward)

                @pl.when(~early & serves & (u == 2 * far) & (t == tiles - 1))
                def _():
                    done_copy(tiles - 1, 1, True).start()

                @pl.when(early & ~at_end & (u == 0) & (t == tiles - 1))
                def _():
                    send_own(SPREAD, inward)

                @pl.when(~early & ~at_end & (u == 0) & (t == soon - 1))
                def _():
                    send_own(SERVED, inward)

                @pl.when(~early & at_end & (u == 0) & (t == tiles - 1))
                def _():
                    query_copy().start()
                    send_own(SERVED, inward)
                    send_own(SPREAD, inward, soon, tiles)

                @pl.when(early & at_end & (u == far) & (t == tiles - 1))
                def _():
                    send_own(SPREAD, inward)

                @pl.when(serving & (s_in == 1) & (t == 0))
                def _():
                    query_copy().wait_recv()

                final = serving & (s_in == far - 1) & (t == tiles - 1)

                @pl.loop(0, jnp.where(serving & ~final, jnp.where(s_in == 1, 3, 1), 0))
                def _(k):
                    owner = jnp.where(k == 2, me, jnp.where(k == 1, from_out, from_in))
                    fold_into(2, end, owner, SERVED, t)

                @pl.when(final)
                def _():
                    finish_served(from_in, t)

                @pl.loop(jnp.where(has_in, 0, 1), jnp.where(both, 4, 2))
                def _(k):
                    outer = (k % 2) == 1

                    @pl.when(jnp.where(outer, has_out, has_in) & ~later)
                    def _():
                        hh = jnp.where(k > 1, SERVED, jnp.where(outer, hh_out, hh_in))
                        fold_into(hh, me, jnp.where(outer, from_out, from_in), hh, t)

    for i in range(tiles):
        for h in range(heads):
            keep(1, i, h)

    @pl.when(~at_end)
    def _():
        for i in range(tiles):
            for h in range(heads):
                keep(0, i, h)

    @pl.when(at_end)
    def _():
        done_copy(tiles - 1, 1, True).wait_recv()
        collect(tiles - 1)
        query_copy().wait_send()

    @pl.when(serves)
    def _():
        done_copy(0, tiles, True).wait_send()

    for step in (1, -1):
        room = jnp.where(step > 0, far - me, me)
        count = n - room

        def sent(ref, row):
            return pltpu.make_async_remote_copy(
                src_ref=ref, dst_ref=ref,
                send_sem=send_sem.at[row, (step + 1) // 2], recv_sem=exit_recv.at[0],
                device_id=peer(step), device_id_type=MESH,
            )

        @pl.when(room == 1)
        def _():
            sent(kv.at[pl.ds(0, far), SPREAD], 0).wait_send()

        for c in range(1, n):
            @pl.when(count == c)
            def _():
                sent(exits.at[pl.ds(0, c)], 1).wait_send()

            if c < far:
                @pl.when(count == c)
                def _():
                    sent(kv.at[pl.ds(0, c)], 0).wait_send()


def write_out(attended, exits, out_hbm, live_hbm, live, sems):
    whole = pltpu.make_async_copy(attended, out_hbm.at[0], sems.at[0])
    whole.start()
    live[0] = jnp.sum((exits[...] > 0).astype(jnp.int32))
    count = pltpu.make_async_copy(live, live_hbm, sems.at[1])
    count.start()
    count.wait()
    whole.wait()


def body(n, queries, keys, values, exit_layer, tile_order):
    rows, q_width = queries.shape[1:]
    kv_width = keys.shape[2]
    q_half = q_width // 2
    heads = q_half // HD
    tiles = rows // TILE
    hbm = pl.BlockSpec(memory_space=pltpu.HBM)
    vmem = pl.BlockSpec(memory_space=pltpu.VMEM)
    dma = pltpu.SemaphoreType.DMA
    attended, exits = pl.pallas_call(
        functools.partial(kernel, n),
        out_shape=(
            pltpu.VMEM((rows, q_width), jnp.bfloat16),
            pltpu.VMEM((n, 1, TILE), jnp.int32),
        ),
        in_specs=[hbm] * 5,
        out_specs=(vmem, vmem),
        scratch_shapes=[
            pltpu.VMEM((3, heads, rows, HD), jnp.bfloat16),
            pltpu.VMEM((n, 2, tiles, 2, TILE, HD), jnp.bfloat16),
            pltpu.VMEM((3, heads * rows, HD), jnp.float32),
            pltpu.VMEM((3, heads * rows, TILE), jnp.float32),
            pltpu.VMEM((2, rows, q_half), jnp.bfloat16),
            pltpu.SMEM(tile_order.shape, jnp.int32),
            pltpu.SMEM(exit_layer.shape, jnp.int32),
            dma((3,)),
            dma((2,)),
            dma((2,)),
            dma((2, 2)),
            dma((n, 2, tiles)),
            dma((2,)),
            dma((3,)),
            dma((n,)),
            pltpu.SemaphoreType.REGULAR,
        ],
        compiler_params=pltpu.CompilerParams(
            collective_id=0, has_side_effects=True, vmem_limit_bytes=62_000_000
        ),
        name="attend_line",
    )(
        tile_order, exit_layer, queries[0],
        keys.reshape(tiles, TILE, kv_width), values.reshape(tiles, TILE, kv_width),
    )
    return pl.pallas_call(
        write_out,
        out_shape=(
            jax.ShapeDtypeStruct((1, rows, q_width), jnp.bfloat16),
            jax.ShapeDtypeStruct((1,), jnp.int32),
        ),
        in_specs=[vmem, vmem],
        out_specs=(hbm, hbm),
        scratch_shapes=[pltpu.SMEM((1,), jnp.int32), dma((2,))],
        compiler_params=pltpu.CompilerParams(vmem_limit_bytes=1_000_000),
        name="write_out",
    )(attended, exits)


def solution(mesh):
    return jax.shard_map(
        functools.partial(body, mesh.shape["seq"]),
        mesh=mesh,
        in_specs=(
            P(None, ("batch", "seq"), "head"),
            P(None, ("batch", "seq"), "head"),
            P(None, ("batch", "seq"), "head"),
            P(("batch", "seq")),
            P("batch"),
        ),
        out_specs=(P(None, ("batch", "seq"), "head"), P("batch")),
        check_vma=False,
    )
```

```python
import functools
import math

import jax
import jax.numpy as jnp
from jax import lax
from jax.experimental import pallas as pl
from jax.experimental.pallas import tpu as pltpu
from jax.sharding import PartitionSpec as P

HD = 256
TILE = 128
SOFTCAP = 50.0
QUERY_SCALE = 0.0625
IN_SCALE = QUERY_SCALE / SOFTCAP
OUT_SCALE = SOFTCAP * math.log2(math.e)
MESH = pl.DeviceIdType.MESH
SERVED, SPREAD = 0, 1
AHEAD = 1


def kernel(
    n, order_hbm, exit_hbm, q_hbm, k_hbm, v_hbm, out_ref, exits,
    qb, kv, acc, den, done, order_ref, exit_ref, kv_sem, q_sem,
    small_sem, send_sem, recv_sem, pair_send, pair_recv, exit_recv, ready,
):
    me = lax.axis_index("seq")
    core = lax.axis_index("head")
    tiles = kv.shape[2]
    heads, rows = qb.shape[1:3]
    q_half = heads * HD
    far = n - 1
    at_end = (me == 0) | (me == far)
    serves = (me == 1) | (me == far - 1)
    end = jnp.where(me < n // 2, 0, far)
    inward = jnp.where(me < n // 2, 1, -1)
    first = core

    def inside(owner):
        return (owner >= 0) & (owner < n)

    def peer(step):
        return {"seq": jnp.clip(me + step, 0, far)}

    def load_own(hh, low, high, sem):
        here = pl.ds(low, high - low)
        for which, src in enumerate((k_hbm, v_hbm)):
            pltpu.make_async_copy(
                src.at[here, :, pl.ds(pl.multiple_of(hh * HD, HD), HD)],
                kv.at[me, hh, here, which],
                kv_sem.at[sem],
            ).start()

    def wait_own(hh, low, high, sem):
        part = kv.at[me, hh, pl.ds(low, high - low)]
        pltpu.make_async_copy(part, part, kv_sem.at[sem]).wait()

    def load_queries(hh):
        for h in range(heads):
            pltpu.make_async_copy(
                q_hbm.at[:, pl.ds(hh * q_half + h * HD, HD)], qb.at[hh, h], q_sem.at[hh]
            ).start()

    def wait_queries(hh):
        pltpu.make_async_copy(qb.at[hh], qb.at[hh], q_sem.at[hh]).wait()

    small = [
        pltpu.make_async_copy(exit_hbm, exit_ref, small_sem.at[0]),
        pltpu.make_async_copy(order_hbm, order_ref, small_sem.at[1]),
    ]

    barrier = pltpu.get_barrier_semaphore()

    @pl.when(inside(me + 1))
    def _():
        pl.semaphore_signal(barrier, inc=1, device_id=peer(1), device_id_type=MESH)

    load_own(first, 0, 1, 2)
    small[0].start()
    asks = at_end & (core == 0)

    @pl.when(asks)
    def _():
        load_queries(0)

    load_own(first, 1, tiles, first)
    @pl.when(inside(me - 1))
    def _():
        pl.semaphore_wait(barrier, 1)
        pl.semaphore_signal(ready, inc=1, device_id=peer(-1), device_id_type=MESH)

    soon = min(AHEAD, tiles - 1)

    def hop(owner, hh, t, step):
        return pltpu.make_async_remote_copy(
            src_ref=kv.at[owner, hh, t],
            dst_ref=kv.at[owner, hh, t],
            send_sem=send_sem.at[0, jnp.where(step > 0, 1, 0)],
            recv_sem=recv_sem.at[owner, hh, t],
            device_id=peer(step),
            device_id_type=MESH,
        )

    def exit_hop(owner, step):
        return pltpu.make_async_remote_copy(
            src_ref=exits.at[owner],
            dst_ref=exits.at[owner],
            send_sem=send_sem.at[1, jnp.where(step > 0, 1, 0)],
            recv_sem=exit_recv.at[owner],
            device_id=peer(step),
            device_id_type=MESH,
        )

    def goes(hh, step):
        room = jnp.where(step > 0, far - me, me)
        return (room > 1) | ((room == 1) & (hh == SPREAD))

    def send(owner, hh, t, step):
        @pl.when(goes(hh, step))
        def _():
            hop(owner, hh, t, step).start()

    def send_own(hh, step, low=0, high=tiles):
        @pl.loop(low, high)
        def _(t):
            send(me, hh, t, step)

    def query_copy():
        return pltpu.make_async_remote_copy(
            src_ref=qb.at[0], dst_ref=qb.at[2],
            send_sem=pair_send.at[0], recv_sem=pair_recv.at[0],
            device_id=peer(inward), device_id_type=MESH,
        )

    def done_copy(low, count, last):
        part = pl.ds(low * TILE, count * TILE)
        return pltpu.make_async_remote_copy(
            src_ref=done.at[0, part], dst_ref=done.at[1, part],
            send_sem=pair_send.at[1], recv_sem=pair_recv.at[2 if last else 1],
            device_id=peer(-inward), device_id_type=MESH,
        )

    def push(step, low, high):
        @pl.when(~at_end)
        def _():
            send_own(first, step, low, high)

        @pl.when(asks)
        def _():
            if low == 0:
                query_copy().start()
            send_own(SERVED, step, low, high)

    @pl.when(asks)
    def _():
        wait_queries(0)

    wait_own(first, 0, 1, 2)

    @pl.when(inside(me - 1))
    def _():
        push(-1, 0, 1)

    small[0].wait()
    lane = lax.broadcasted_iota(jnp.int32, (1, TILE), 1)
    mine = jnp.zeros((1, TILE), jnp.int32)
    for i in range(tiles):
        mine = jnp.where(lane == i, exit_ref[i], mine)
    exits[me] = mine

    @pl.when(inside(me - 1))
    def _():
        exit_hop(me, -1).start()

    wait_own(first, 1, tiles, first)

    @pl.when(inside(me - 1))
    def _():
        push(-1, 1, tiles)

    @pl.when(inside(me + 1))
    def _():
        pl.semaphore_wait(ready, 1)
        exit_hop(me, 1).start()
        push(1, 0, tiles)

    @pl.when(at_end & (core == 1))
    def _():
        send_own(SPREAD, inward, 0, soon)

    load_own(1 - first, 0, tiles, 1 - first)
    load_queries(1)
    small[1].start()

    @pl.when(~asks)
    def _():
        load_queries(0)

    wait_own(1 - first, 0, tiles, 1 - first)

    @pl.when(~at_end)
    def _():
        send_own(1 - first, -inward)

    acc[...] = jnp.zeros_like(acc)
    den[...] = jnp.zeros_like(den)

    @pl.when(~asks)
    def _():
        wait_queries(0)

    wait_queries(1)
    small[1].wait()
    ahead = lax.broadcasted_iota(jnp.int32, (TILE, TILE), 1) - lax.broadcasted_iota(
        jnp.int32, (TILE, TILE), 0
    )

    def fold_into(slot, row_owner, owner, hh, t):
        key_place = order_ref[owner * tiles + t]
        parts = []
        for h in range(heads):
            for i in range(tiles):
                here = pl.ds(h * rows + i * TILE, TILE)
                gap = (order_ref[row_owner * tiles + i] - key_place) * TILE
                scores = lax.dot_general(
                    qb[slot, h, pl.ds(i * TILE, TILE), :], kv[owner, hh, t, 0],
                    (((1,), (1,)), ((), ())), preferred_element_type=jnp.float32,
                )
                weights = jnp.where(
                    ahead <= gap, jnp.exp2(OUT_SCALE * jnp.tanh(scores * IN_SCALE)), 0.0
                )
                den[slot, here, :] += weights
                parts.append(weights.astype(jnp.bfloat16))
        acc[slot] += jnp.dot(
            jnp.concatenate(parts, axis=0), kv[owner, hh, t, 1],
            preferred_element_type=jnp.float32,
        )

    def finish(slot, i, h):
        here = pl.ds(h * rows + i * TILE, TILE)
        total = jnp.sum(den[slot, here, :], axis=1, keepdims=True)
        return (acc[slot, here, :] / total).astype(jnp.bfloat16)

    def live_only(i, rows_out):
        return jnp.where(exit_ref[i] > 0, rows_out, jnp.zeros_like(rows_out))

    def keep(slot, i, h):
        out_ref[pl.ds(i * TILE, TILE), pl.ds(slot * q_half + h * HD, HD)] = live_only(
            i, finish(slot, i, h)
        )

    @pl.loop(jnp.where(at_end, tiles * (1 - core), 0), jnp.where(at_end, tiles * (2 - core), 2 * tiles))
    def _(k):
        hh = jnp.where(k < tiles, first, 1 - first)
        fold_into(hh, me, me, hh, lax.rem(k, tiles))

    def arrive(owner, hh, t, side):
        hop(owner, hh, t, side).wait_recv()
        send(owner, hh, t, -side)

        @pl.when((hh == SPREAD) & (t == 0))
        def _():
            exit_hop(owner, side).wait_recv()

            @pl.when(inside(me - side))
            def _():
                exit_hop(owner, -side).start()

    def collect(i):
        here = pl.ds(i * TILE, TILE)
        out_ref[here, pl.ds(0, q_half)] = live_only(i, done[1, here, :])

    def finish_served(owner, t):
        key_place = order_ref[owner * tiles + t]
        for i in range(tiles):
            place = order_ref[end * tiles + i]
            part = pl.ds(i * TILE, TILE)
            scores = lax.dot_general(
                qb[2, :, part, :].reshape(heads * TILE, HD), kv[owner, SERVED, t, 0],
                (((1,), (1,)), ((), ())), preferred_element_type=jnp.float32,
            ).reshape(heads, TILE, TILE)
            weights = jnp.where(
                (ahead - (place - key_place) * TILE)[None] <= 0,
                jnp.exp2(OUT_SCALE * jnp.tanh(scores * IN_SCALE)), 0.0,
            )
            added = jnp.dot(
                weights.astype(jnp.bfloat16).reshape(heads * TILE, TILE),
                kv[owner, SERVED, t, 1], preferred_element_type=jnp.float32,
            ).reshape(heads, TILE, HD)
            for h in range(heads):
                here = pl.ds(h * rows + i * TILE, TILE)
                total = jnp.sum(den[2, here, :] + weights[h], axis=1, keepdims=True)
                done[0, part, pl.ds(h * HD, HD)] = (
                    (acc[2, here, :] + added[h]) / total
                ).astype(jnp.bfloat16)
            if i > 0:
                done_copy(i - 1, 1, False).start()

        @pl.when(core == 0)
        def _():
            for h in range(heads):
                keep(0, 0, h)
            done_copy(tiles - 1, 1, True).start()

    early = core == 0

    @pl.loop(0, 3 * far - 1)
    def _(u):
        spread_a = u >= far
        s_a = jnp.where(spread_a, u - far + 1, u + 1)
        served_b = (u >= far) & (u < 2 * far)
        late_b = u >= 2 * far
        s_b = jnp.where(late_b, u - 2 * far + 2, jnp.where(served_b, u - far + 1, u + 1))
        hh_in = jnp.where(early, spread_a, ~served_b).astype(jnp.int32)
        s_in = jnp.where(early, s_a, s_b)
        extra = serves & (u == far + 1)
        hh_out = jnp.where(early, spread_a, ~served_b | extra).astype(jnp.int32)
        s_out = jnp.where(early, s_a, jnp.where(extra, 1, jnp.where(late_b, s_b - 1, s_b)))
        part_in = ~early & (u > 0) & (hh_in == SPREAD)
        low_in = jnp.where(part_in & late_b, soon, 0)
        high_in = jnp.where(part_in & ~late_b, soon, tiles)
        part_out = ~early & (hh_out == SPREAD)
        low_out = jnp.where(part_out & (late_b | extra), soon, 0)
        high_out = jnp.where(part_out & ~(late_b | extra), soon, tiles)
        from_in = me + inward * s_in
        from_out = me - inward * s_out
        runs = ~early | (u < 2 * far)
        any_in = runs & inside(from_in) & ~(at_end & (hh_in == SERVED))
        any_out = runs & inside(from_out) & ~at_end & ~(late_b & ~early & serves)
        later = early & ~at_end & (hh_in == SERVED)
        both = early & ~at_end & (hh_in == SPREAD)
        serving = runs & serves & (hh_in == SERVED) & inside(from_in)

        @pl.when(any_in | any_out)
        def _():
            @pl.loop(0, tiles)
            def _(t):
                has_in = any_in & (t >= low_in) & (t < high_in)
                has_out = any_out & (t >= low_out) & (t < high_out)

                @pl.when((u == jnp.where(early, 2 * far - 1, 3 * far - 2)) & (t == tiles - 1) & at_end)
                def _():
                    done_copy(0, tiles - 1, False).wait_recv()
                    for i in range(tiles - 1):
                        collect(i)

                @pl.when(has_out)
                def _():
                    arrive(from_out, hh_out, t, -inward)

                @pl.when(has_in)
                def _():
                    arrive(from_in, hh_in, t, inward)

                @pl.when(~early & serves & (u == 2 * far) & (t == tiles - 1))
                def _():
                    done_copy(tiles - 1, 1, True).start()

                @pl.when(early & ~at_end & (u == 0) & (t == tiles - 1))
                def _():
                    send_own(SPREAD, inward)

                @pl.when(~early & ~at_end & (u == 0) & (t == soon - 1))
                def _():
                    send_own(SERVED, inward)

                @pl.when(~early & at_end & (u == 0) & (t == tiles - 1))
                def _():
                    query_copy().start()
                    send_own(SERVED, inward)
                    send_own(SPREAD, inward, soon, tiles)

                @pl.when(early & at_end & (u == far) & (t == tiles - 1))
                def _():
                    send_own(SPREAD, inward)

                @pl.when(serving & (s_in == 1) & (t == 0))
                def _():
                    query_copy().wait_recv()

                final = serving & (s_in == far - 1) & (t == tiles - 1)

                @pl.loop(0, jnp.where(serving & ~final, jnp.where(s_in == 1, 3, 1), 0))
                def _(k):
                    owner = jnp.where(k == 2, me, jnp.where(k == 1, from_out, from_in))
                    fold_into(2, end, owner, SERVED, t)

                @pl.when(final)
                def _():
                    finish_served(from_in, t)

                @pl.loop(jnp.where(has_in, 0, 1), jnp.where(both, 4, 2))
                def _(k):
                    outer = (k % 2) == 1

                    @pl.when(jnp.where(outer, has_out, has_in) & ~later)
                    def _():
                        hh = jnp.where(k > 1, SERVED, jnp.where(outer, hh_out, hh_in))
                        fold_into(hh, me, jnp.where(outer, from_out, from_in), hh, t)

    for i in range(tiles):
        for h in range(heads):
            keep(1, i, h)

    @pl.when(~at_end)
    def _():
        for i in range(tiles):
            for h in range(heads):
                keep(0, i, h)

    @pl.when(at_end)
    def _():
        done_copy(tiles - 1, 1, True).wait_recv()
        collect(tiles - 1)
        query_copy().wait_send()

    @pl.when(serves)
    def _():
        done_copy(0, tiles, True).wait_send()

    for step in (1, -1):
        room = jnp.where(step > 0, far - me, me)
        count = n - room

        def sent(ref, row):
            return pltpu.make_async_remote_copy(
                src_ref=ref, dst_ref=ref,
                send_sem=send_sem.at[row, (step + 1) // 2], recv_sem=exit_recv.at[0],
                device_id=peer(step), device_id_type=MESH,
            )

        @pl.when(room == 1)
        def _():
            sent(kv.at[pl.ds(0, far), SPREAD], 0).wait_send()

        for c in range(1, n):
            @pl.when(count == c)
            def _():
                sent(exits.at[pl.ds(0, c)], 1).wait_send()

            if c < far:
                @pl.when(count == c)
                def _():
                    sent(kv.at[pl.ds(0, c)], 0).wait_send()


def write_out(attended, exits, out_hbm, live_hbm, live, sems):
    whole = pltpu.make_async_copy(attended, out_hbm.at[0], sems.at[0])
    whole.start()
    live[0] = jnp.sum((exits[...] > 0).astype(jnp.int32))
    count = pltpu.make_async_copy(live, live_hbm, sems.at[1])
    count.start()
    count.wait()
    whole.wait()


def body(n, queries, keys, values, exit_layer, tile_order):
    rows, q_width = queries.shape[1:]
    kv_width = keys.shape[2]
    q_half = q_width // 2
    heads = q_half // HD
    tiles = rows // TILE
    hbm = pl.BlockSpec(memory_space=pltpu.HBM)
    vmem = pl.BlockSpec(memory_space=pltpu.VMEM)
    dma = pltpu.SemaphoreType.DMA
    attended, exits = pl.pallas_call(
        functools.partial(kernel, n),
        out_shape=(
            pltpu.VMEM((rows, q_width), jnp.bfloat16),
            pltpu.VMEM((n, 1, TILE), jnp.int32),
        ),
        in_specs=[hbm] * 5,
        out_specs=(vmem, vmem),
        scratch_shapes=[
            pltpu.VMEM((3, heads, rows, HD), jnp.bfloat16),
            pltpu.VMEM((n, 2, tiles, 2, TILE, HD), jnp.bfloat16),
            pltpu.VMEM((3, heads * rows, HD), jnp.float32),
            pltpu.VMEM((3, heads * rows, TILE), jnp.float32),
            pltpu.VMEM((2, rows, q_half), jnp.bfloat16),
            pltpu.SMEM(tile_order.shape, jnp.int32),
            pltpu.SMEM(exit_layer.shape, jnp.int32),
            dma((3,)),
            dma((2,)),
            dma((2,)),
            dma((2, 2)),
            dma((n, 2, tiles)),
            dma((2,)),
            dma((3,)),
            dma((n,)),
            pltpu.SemaphoreType.REGULAR,
        ],
        compiler_params=pltpu.CompilerParams(
            collective_id=0, has_side_effects=True, vmem_limit_bytes=62_000_000
        ),
        name="attend_line",
    )(
        tile_order, exit_layer, queries[0],
        keys.reshape(tiles, TILE, kv_width), values.reshape(tiles, TILE, kv_width),
    )
    return pl.pallas_call(
        write_out,
        out_shape=(
            jax.ShapeDtypeStruct((1, rows, q_width), jnp.bfloat16),
            jax.ShapeDtypeStruct((1,), jnp.int32),
        ),
        in_specs=[vmem, vmem],
        out_specs=(hbm, hbm),
        scratch_shapes=[pltpu.SMEM((1,), jnp.int32), dma((2,))],
        compiler_params=pltpu.CompilerParams(vmem_limit_bytes=1_000_000),
        name="write_out",
    )(attended, exits)


def solution(mesh):
    return jax.shard_map(
        functools.partial(body, mesh.shape["seq"]),
        mesh=mesh,
        in_specs=(
            P(None, ("batch", "seq"), "head"),
            P(None, ("batch", "seq"), "head"),
            P(None, ("batch", "seq"), "head"),
            P(("batch", "seq")),
            P("batch"),
        ),
        out_specs=(P(None, ("batch", "seq"), "head"), P("batch")),
        check_vma=False,
    )
```
